32 devices in a mesh: band: 8 (over z, x), ga: 4 (over y, core).
Axes of the slice: x: 2, y: 2, z: 4, core: 2. Of those that a mesh axis runs over, the one named last changes fastest.
Arguments:
- elements: bfloat16 [2, 768, 2048], P(None, 'band', 'ga'), may hold values from -0.75 to 0.75
- screened: bfloat16 [2, 2, 2048, 2048], P(None, None, 'ga'), may hold values from -0.09375 to 0.09375
- energies: float32 [768], replicated, may hold values from -3 to 3
- freq_points: float32 [2], replicated, may hold values from -3 to 3
- freq_weights: float32 [2], replicated, may hold values from 0.5 to 2
- band_of_slot: int32 [768], replicated, may hold values from 0 to 767, each once
Outputs:
- sigma: float32 [2, 768, 768], P(None, 'band', 'ga')
The draws below stay inside these ranges and needn't reach their ends.
Inputs may be any that keep to these rules, and one draw needn't show every extreme that they name: `band_of_slot`: each of 0 to 767 stands once.
All inputs are finite; a program needn't handle non-finite values.
Results may differ from the reference program's by a relative error of at most 0.0042.
Values may be sent and summed in bfloat16 or wider, within the bound.
A program may use at most 128 MiB of HBM per device.

```python
import math
import jax
import jax.numpy as jnp

NG = 2048
NW = 2
NB = 768


def block_levels(rng, extent, split, smallest, high):
    gain = 1.0
    for axis_at, blocks in split:
        heights = jax.random.uniform(jax.random.fold_in(jax.random.fold_in(rng, 6), axis_at), (blocks,), jnp.float32, smallest / len(split), high / len(split))
        gain = gain * jnp.repeat(jnp.exp(heights), extent[axis_at] // blocks).reshape((-1,) + (1,) * (len(extent) - 1 - axis_at))
    return gain


def normal_values(rng, dims, deviation, limit, shards=(), dtype=jnp.bfloat16):
    values = deviation * jax.random.normal(rng, dims, jnp.float32)
    if shards:
        values = values * block_levels(rng, dims, shards, -0.22, 0.18)
    return jnp.clip(values, -limit, limit).astype(dtype)


def setup_inputs(seed: int = 0) -> dict:
    keys = jax.random.split(jax.random.key(seed), 7)
    elements = normal_values(keys[0], (2, NB, NG), 0.125, 0.75, ((1, 8), (2, 4)))
    screened = normal_values(keys[1], (NW, 2, NG, NG), (2 * NG) ** -0.5, 0.09375, ((2, 4),))
    energies = jnp.clip(jax.random.uniform(keys[2], (NB,), jnp.float32, -3.0, 3.0), -3.0, 3.0)
    freq_points = jnp.clip(jax.random.uniform(keys[3], (NW,), jnp.float32, -3.0, 3.0), -3.0, 3.0)
    freq_weights = jnp.clip(jnp.exp(jax.random.uniform(keys[4], (NW,), jnp.float32, math.log(0.5), math.log(2.0))), 0.5, 2.0)
    band_of_slot = jax.random.permutation(keys[5], NB).astype(jnp.int32)
    return dict(elements=elements, screened=screened, energies=energies, freq_points=freq_points, freq_weights=freq_weights, band_of_slot=band_of_slot)


def reference(elements, screened, energies, freq_points, freq_weights, band_of_slot):
    slot_energy = jnp.take(energies, band_of_slot.astype(jnp.int32))
    offset = slot_energy[None, :] - freq_points[:, None]
    screen = freq_weights[:, None] / (1.0 + 4.0 * offset * offset)
    real_part = elements[0]
    imag_part = elements[1]
    total = jnp.zeros((2, NB, NB), jnp.float32)
    for freq in range(NW):
        w_real = screened[freq, 0]
        w_imag = screened[freq, 1]
        y_real = (jnp.dot(real_part, w_real.T, preferred_element_type=jnp.float32)
                  - jnp.dot(imag_part, w_imag.T, preferred_element_type=jnp.float32)).astype(jnp.bfloat16)
        y_imag = (jnp.dot(real_part, w_imag.T, preferred_element_type=jnp.float32)
                  + jnp.dot(imag_part, w_real.T, preferred_element_type=jnp.float32)).astype(jnp.bfloat16)
        pair_real = (jnp.dot(real_part, y_real.T, preferred_element_type=jnp.float32)
                     + jnp.dot(imag_part, y_imag.T, preferred_element_type=jnp.float32))
        pair_imag = (jnp.dot(real_part, y_imag.T, preferred_element_type=jnp.float32)
                     - jnp.dot(imag_part, y_real.T, preferred_element_type=jnp.float32))
        factor = 0.5 * (screen[freq][:, None] + screen[freq][None, :])
        total = total + factor[None] * jnp.stack([pair_real, pair_imag])
    return total
```

```python
import functools

import jax
import jax.numpy as jnp
from jax import lax
from jax.experimental import pallas as pl
from jax.experimental.pallas import tpu as pltpu
from jax.sharding import PartitionSpec as P

MESH = pl.DeviceIdType.MESH
F32 = jnp.float32
BF16 = jnp.bfloat16
NT = (((1,), (1,)), ((), ()))
NX = 2
CHIPS = 4


def kernel(nb, ng, el, wh, en_h, bos_h, fp_h, fw_h, out, *scratch):
    (en, bos, fp, fw, mine, gat, wv, a_ref, e3, scr, held, dsend, drecv, ysend, yrecv, xsend, lv, lw, ssend, srecv, own,
     in_sem, loc_sem, w_sem, sw_ss, up_sem, dn_sem, g_recv, d_ss, d_rs, y_ss, y_rs, x_ss, x_rs, l_ss, l_rs, s_ss,
     s_rs) = scratch
    rows, depth = el.shape[1], el.shape[2]
    nz = nb // NX
    per = nb // ng
    slots = en.shape[0]
    b, g = lax.axis_index("band"), lax.axis_index("ga")
    z, x = b // NX, lax.rem(b, NX)
    y, c = g // 2, lax.rem(g, 2)
    mate = g + 1 - 2 * c
    across = lax.rem(g + 2, ng)
    xb = b + 1 - 2 * x
    straight = x == c
    crossed = x != c

    barrier = pltpu.get_barrier_semaphore()

    def greet(band, ga):
        pl.semaphore_signal(barrier, inc=1, device_id=(band, ga), device_id_type=MESH)

    @pl.when(z > 0)
    def _():
        greet(b - NX, g)

    @pl.when(z < nz - 1)
    def _():
        greet(b + NX, g)

    greet(xb, g)
    for r in range(1, ng):
        greet(b, lax.rem(g + r, ng))
        greet(xb, lax.rem(g + r, ng))

    small = [pltpu.make_async_copy(s, t, in_sem.at[i]) for i, (s, t) in enumerate(
        ((en_h, en), (bos_h, bos), (fp_h, fp), (fw_h, fw)))]
    local = pltpu.make_async_copy(el, mine, loc_sem.at[0])
    local.start()

    def placed():
        return pltpu.make_async_copy(el, gat.at[:, pl.ds(pl.multiple_of(z * rows, rows), rows), :], loc_sem.at[1])

    @pl.when(straight)
    def _():
        placed().start()

    for copy in small:
        copy.start()

    def slice_of(j):
        ys = 1 - y if j < 2 else y
        xs = x if j % 2 else 1 - x
        return ys * 2 + xs

    def w_copy(j, o):
        w = c if o else 1 - c
        cols = pl.ds(pl.multiple_of(slice_of(j) * depth, depth), depth)
        return pltpu.make_async_copy(wh.at[w, :, :, cols], wv.at[o, j], w_sem.at[o, j])

    order = ((0, 0), (1, 0), (0, 1), (1, 1), (2, 0), (3, 0), (2, 1), (3, 1))
    local.wait()

    @pl.when(straight)
    def _():
        placed().wait()

    below = jnp.where(z > 0, 1, 0)
    above = jnp.where(z < nz - 1, 1, 0)
    pl.semaphore_wait(barrier, 2 * ng - 1 + below + above)

    unit = rows // 6
    pieces = ((0, 2 * unit), (2 * unit, 2 * unit), (4 * unit, unit), (5 * unit, unit))
    parts = range(len(pieces))

    def block(zs, i):
        start, size = pieces[i]
        return gat.at[:, pl.ds(pl.multiple_of(zs * rows + start, unit), size), :]

    def send(zs, i, band, sem):
        ref = block(zs, i)
        return pltpu.make_async_remote_copy(
            src_ref=ref, dst_ref=ref, send_sem=sem, recv_sem=g_recv.at[zs, i], device_id=(band, g), device_id_type=MESH)

    def swap(i):
        start, size = pieces[i]
        return pltpu.make_async_remote_copy(
            src_ref=mine.at[:, pl.ds(start, size), :], dst_ref=block(z, i), send_sem=sw_ss.at[i],
            recv_sem=g_recv.at[z, i], device_id=(xb, mate), device_id_type=MESH)

    def arrived(zs, i):
        send(zs, i, b, up_sem.at[zs, i]).wait_recv()

    def send_z(zs, i, up, down):
        if up:
            @pl.when(z < nz - 1)
            def _():
                send(zs, i, b + NX, up_sem.at[zs, i]).start()

        if down:
            @pl.when(z > 0)
            def _():
                send(zs, i, b - NX, dn_sem.at[zs, i]).start()

    def fwd(s, which=parts):
        for i in which:
            for zs, up in ((z - s, True), (z + s, False)):
                @pl.when((zs >= 0) & (zs < nz))
                def _():
                    arrived(zs, i)
                    send_z(zs, i, up, not up)

    def swapped(which):
        @pl.when(crossed)
        def _():
            for i in which:
                arrived(z, i)
                send_z(z, i, True, True)

    @pl.when(straight)
    def _():
        for i in parts:
            send_z(z, i, True, True)

    @pl.when(crossed)
    def _():
        for i in parts:
            swap(i).start()

    for j, o in order:
        w_copy(j, o).start()

    for copy in small:
        copy.wait()
    row = lax.broadcasted_iota(jnp.int32, (16, slots), 0)
    e = en[...].reshape(1, slots)
    hi = e.astype(BF16).astype(F32)
    mid = (e - hi).astype(BF16).astype(F32)
    lo = e - hi - mid
    e3[...] = jnp.where(row == 0, hi, jnp.where(row == 1, mid, jnp.where(row == 2, lo, 0.0))).astype(BF16)
    tile = slots if slots <= 1024 else 8 * rows

    for u in range(slots // tile):
        slot = bos[u * tile : (u + 1) * tile].reshape(1, tile)

        def add(j, acc):
            at = pl.multiple_of(j * tile, tile)
            hit = lax.broadcasted_iota(jnp.int32, (tile, tile), 0) + at == slot
            return acc + jnp.dot(e3[:, pl.ds(at, tile)], jnp.where(hit, 1.0, 0.0).astype(BF16),
                                 preferred_element_type=F32)

        acc = lax.fori_loop(0, slots // tile, add, jnp.zeros((16, tile), F32))
        energy = jnp.sum(acc, axis=0, keepdims=True)
        for w in range(2):
            off = energy - fp[w]
            value = 0.5 * (fw[w] / (1.0 + 4.0 * off * off))
            for v in range(tile // rows):
                scr[u * (tile // rows) + v, w : w + 1, :] = value[:, v * rows : (v + 1) * rows]
    pick = lax.broadcasted_iota(jnp.int32, (rows, rows), 1) == lax.broadcasted_iota(
        jnp.int32, (rows, rows), 0)
    cols = [[jnp.sum(jnp.where(pick, scr[z * NX + v, w : w + 1, :], 0.0), axis=1, keepdims=True)
             for w in range(2)] for v in range(NX)]

    er = mine[0]
    ei = mine[1]
    a_ref[:rows, :depth] = er
    a_ref[:rows, depth:] = ei
    a_ref[rows:, :depth] = -ei
    a_ref[rows:, depth:] = er

    def d_copy(j):
        return pltpu.make_async_remote_copy(
            src_ref=dsend.at[j], dst_ref=drecv.at[j], send_sem=d_ss.at[j], recv_sem=d_rs.at[j],
            device_id=(b, mate), device_id_type=MESH)

    def y_copy(j, h):
        return pltpu.make_async_remote_copy(
            src_ref=ysend.at[j, h], dst_ref=yrecv.at[j, h], send_sem=y_ss.at[j, h], recv_sem=y_rs.at[j, h],
            device_id=(b, across), device_id_type=MESH)

    def x_copy(h):
        return pltpu.make_async_remote_copy(
            src_ref=xsend.at[h], dst_ref=lv.at[x, c, h], send_sem=x_ss.at[h], recv_sem=x_rs.at[h],
            device_id=(xb, g), device_id_type=MESH)

    def l_copy(v, band, h):
        ref = lv.at[band, c, h]
        return pltpu.make_async_remote_copy(
            src_ref=ref, dst_ref=ref, send_sem=l_ss.at[v, h], recv_sem=l_rs.at[v, h],
            device_id=(b, mate), device_id_type=MESH)

    def first(j, o):
        w_copy(j, o).wait()
        part = jnp.dot(a_ref[...], wv[o, j].reshape(2 * depth, depth), preferred_element_type=F32)
        if not o:
            dsend[j] = part.astype(BF16)
            d_copy(j).start()
            return
        d_copy(j).wait_recv()
        part = part + drecv[j].astype(F32)
        for h in range(2):
            if j < 2:
                ysend[j, h] = part[h * rows : (h + 1) * rows].astype(BF16)
                y_copy(j, h).start()
            else:
                held[j - 2, h] = part[h * rows : (h + 1) * rows]

    def to_x(h):
        y_copy(0, h).wait_recv()
        xsend[h] = (held[0, h] + yrecv[0, h].astype(F32)).astype(BF16)
        x_copy(h).start()

    def here(h):
        y_copy(1, h).wait_recv()
        lv[x, c, h] = (held[1, h] + yrecv[1, h].astype(F32)).astype(BF16)
        l_copy(0, x, h).start()

    def from_x(h):
        x_copy(h).wait_recv()
        l_copy(1, 1 - x, h).start()

    def consume_block(zs):
        at = pl.ds(pl.multiple_of(zs * rows, rows), rows)
        k = zs * NX + c
        pr = lax.dot_general(lv[...].reshape(8 * rows, depth), gat[0, at, :], NT, preferred_element_type=F32)
        pr = pr + lax.dot_general(lw[...].reshape(8 * rows, depth), gat[1, at, :], NT, preferred_element_type=F32)
        q, p = k // per, lax.rem(k, per)
        srow = [scr[k, w : w + 1, :] for w in range(2)]
        for v in range(NX):
            f = [cols[v][w] + srow[w] for w in range(2)]
            base = 4 * v * rows
            total = [f[0] * pr[base + i * rows : base + (i + 1) * rows]
                     + f[1] * pr[base + (2 + i) * rows : base + (3 + i) * rows] for i in range(2)]
            home = (q == g) & (x == v)

            @pl.when(home)
            def _():
                for i in range(2):
                    own[p, i] = total[i]
                    srecv[x * 2 + y, p, i] = jnp.zeros((rows, rows), BF16)

            @pl.when(jnp.logical_not(home))
            def _():
                for i in range(2):
                    ssend[zs, v, i] = total[i].astype(BF16)
                pltpu.make_async_remote_copy(
                    src_ref=ssend.at[zs, v], dst_ref=srecv.at[x * 2 + y, p], send_sem=s_ss.at[zs, v],
                    recv_sem=s_rs.at[x * 2 + y, p], device_id=(z * NX + v, q), device_id_type=MESH).start()

    def consume(s):
        @pl.when(z - s >= 0)
        def _():
            consume_block(z - s)

        if not (isinstance(s, int) and s == 0):
            @pl.when(z + s < nz)
            def _():
                consume_block(z + s)

    first(0, 0)
    first(1, 0)
    first(0, 1)
    first(1, 1)
    swapped((0, 1))
    first(2, 0)
    first(3, 0)
    swapped((2, 3))
    fwd(1, (0,))
    first(2, 1)
    first(3, 1)
    own[...] = jnp.zeros(own.shape, F32)
    fwd(1, (1,))
    to_x(0)
    fwd(1, (2, 3))
    to_x(1)
    fwd(2, (0,))
    from_x(0)
    fwd(2, (1,))
    here(0)
    from_x(1)
    fwd(2, (2, 3))
    here(1)
    fwd(3, (0,))
    for v in range(2):
        for h in range(2):
            l_copy(v, x, h).wait_recv()
    for v in range(NX):
        for w in range(2):
            lw[v, w, 0] = -lv[v, w, 1]
            lw[v, w, 1] = lv[v, w, 0]
    consume(0)
    consume(1)
    fwd(3, (1,))
    consume(2)
    fwd(3, (2, 3))
    consume(3)

    def tail(s, carry):
        fwd(s)
        consume(s)
        return carry

    lax.fori_loop(4, nz, tail, 0)

    chip = x * 2 + y
    for p in range(per):
        for r in range(CHIPS):
            @pl.when(jnp.logical_not((chip == r) & (c == p % 2)))
            def _():
                pltpu.make_async_remote_copy(
                    src_ref=ssend.at[0, 0], dst_ref=srecv.at[r, p], send_sem=s_ss.at[0, 0], recv_sem=s_rs.at[r, p],
                    device_id=(b, mate), device_id_type=MESH).wait_recv()
        for i in range(2):
            total = own[p, i]
            for r in range(CHIPS):
                total = total + srecv[r, p, i].astype(F32)
            out[i, :, p * rows : (p + 1) * rows] = total

    def sent(zs, carry):
        for i in parts:
            @pl.when((zs <= z) & (z < nz - 1))
            def _():
                send(zs, i, b, up_sem.at[zs, i]).wait_send()

            @pl.when((zs >= z) & (z > 0))
            def _():
                send(zs, i, b, dn_sem.at[zs, i]).wait_send()

        q = (zs * NX + c) // per
        for v in range(NX):
            @pl.when((q != g) | (x != v))
            def _():
                pltpu.make_async_remote_copy(
                    src_ref=ssend.at[zs, v], dst_ref=srecv.at[0, 0], send_sem=s_ss.at[zs, v], recv_sem=s_rs.at[0, 0],
                    device_id=(b, mate), device_id_type=MESH).wait_send()

        return carry

    lax.fori_loop(0, nz, sent, 0)

    @pl.when(crossed)
    def _():
        for i in parts:
            swap(i).wait_send()

    for j in range(4):
        d_copy(j).wait_send()
    for h in range(2):
        for j in range(2):
            y_copy(j, h).wait_send()
            l_copy(j, x, h).wait_send()
        x_copy(h).wait_send()


def solution(mesh):
    nb, ng = mesh.shape["band"], mesh.shape["ga"]
    nz = nb // NX
    per = nb // ng

    def step(elements, screened, energies, freq_points, freq_weights, band_of_slot):
        _, rows, depth = elements.shape
        slots = energies.shape[0]
        any_space = pl.BlockSpec(memory_space=pl.ANY)
        vmem = pl.BlockSpec(memory_space=pltpu.VMEM)
        dma = pltpu.SemaphoreType.DMA
        return pl.pallas_call(
            functools.partial(kernel, nb, ng),
            out_shape=pltpu.VMEM((2, rows, per * rows), F32),
            in_specs=[any_space] * 6,
            out_specs=vmem,
            scratch_shapes=[
                pltpu.VMEM((slots,), F32), pltpu.VMEM((slots,), jnp.int32),
                pltpu.SMEM(freq_points.shape, F32), pltpu.SMEM(freq_weights.shape, F32),
                pltpu.VMEM((2, rows, depth), BF16),
                pltpu.VMEM((2, nz * rows, depth), BF16),
                pltpu.VMEM((2, 4, 2, depth, depth), BF16),
                pltpu.VMEM((2 * rows, 2 * depth), BF16),
                pltpu.VMEM((16, slots), BF16),
                pltpu.VMEM((nb, 2, rows), F32),
                pltpu.VMEM((2, 2, rows, depth), F32),
                pltpu.VMEM((4, 2 * rows, depth), BF16),
                pltpu.VMEM((4, 2 * rows, depth), BF16),
                pltpu.VMEM((2, 2, rows, depth), BF16),
                pltpu.VMEM((2, 2, rows, depth), BF16),
                pltpu.VMEM((2, rows, depth), BF16),
                pltpu.VMEM((NX, 2, 2, rows, depth), BF16),
                pltpu.VMEM((NX, 2, 2, rows, depth), BF16),
                pltpu.VMEM((nz, NX, 2, rows, rows), BF16),
                pltpu.VMEM((CHIPS, per, 2, rows, rows), BF16),
                pltpu.VMEM((per, 2, rows, rows), F32),
                dma((4,)), dma((2,)), dma((2, 4)), dma((4,)), dma((nz, 4)), dma((nz, 4)), dma((nz, 4)),
                dma((4,)), dma((4,)), dma((2, 2)), dma((2, 2)), dma((2,)), dma((2,)), dma((2, 2)), dma((2, 2)),
                dma((nz, NX)), dma((CHIPS, per)),
            ],
            compiler_params=pltpu.CompilerParams(
                collective_id=0, has_side_effects=True, vmem_limit_bytes=60 * 1024 * 1024),
        )(elements, screened, energies, band_of_slot, freq_points, freq_weights)

    placed = (P(None, "band", "ga"), P(None, None, "ga", None), P(), P(), P(), P())
    return jax.shard_map(
        step, mesh=mesh, in_specs=placed, out_specs=P(None, "band", "ga"), check_vma=False
    )
```

```python
import functools

import jax
import jax.numpy as jnp
from jax import lax
from jax.experimental import pallas as pl
from jax.experimental.pallas import tpu as pltpu
from jax.sharding import PartitionSpec as P

MESH = pl.DeviceIdType.MESH
F32 = jnp.float32
BF16 = jnp.bfloat16
NT = (((1,), (1,)), ((), ()))
NX = 2
CUTS = 4
LANES = 128
CHIPS = 4


def packs(rows):
    return 2 * (2 * rows - LANES) == LANES


def pack(re, im):
    rows = re.shape[0]
    if not packs(rows):
        return jnp.concatenate([re, im], axis=0)
    spare = LANES - rows
    top = jnp.concatenate([re, im[:, :spare]], axis=1)
    rest = im[:, spare:]
    return jnp.concatenate([top, jnp.concatenate([rest[: rows // 2], rest[rows // 2 :]], axis=1)], axis=0)


def unpack(both, rows):
    if not packs(rows):
        return both[:rows], both[rows:]
    rest = both[rows:]
    rest = jnp.concatenate([rest[:, : LANES // 2], rest[:, LANES // 2 :]], axis=0)
    return both[:rows, :rows], jnp.concatenate([both[:rows, rows:], rest], axis=1)


def kernel(nb, ng, el, wh, en_h, bos_h, fp_h, fw_h, out, *scratch):
    (en, bos, fp, fw, mine, gat, wv, a_ref, e3, scr, held, dsend, drecv, ysend, yrecv, xsend, lv, lw, ssend, srecv, own,
     in_sem, loc_sem, w_sem, sw_ss, up_sem, dn_sem, g_recv, d_ss, d_rs, y_ss, y_rs, x_ss, x_rs, l_ss, l_rs, s_ss,
     s_rs) = scratch
    rows, depth = el.shape[1], el.shape[2]
    nz = nb // NX
    pad = gat.shape[1] // nz
    cut = 2 * rows // CUTS
    per = nb // ng
    slots = en.shape[0]
    b, g = lax.axis_index("band"), lax.axis_index("ga")
    z, x = b // NX, lax.rem(b, NX)
    y, c = g // 2, lax.rem(g, 2)
    mate = g + 1 - 2 * c
    across = lax.rem(g + 2, ng)
    xb = b + 1 - 2 * x
    straight = x == c
    crossed = x != c

    barrier = pltpu.get_barrier_semaphore()

    def greet(band, ga):
        pl.semaphore_signal(barrier, inc=1, device_id=(band, ga), device_id_type=MESH)

    @pl.when(z > 0)
    def _():
        greet(b - NX, g)

    @pl.when(z < nz - 1)
    def _():
        greet(b + NX, g)

    greet(xb, g)
    greet(xb, mate)
    for r in range(1, ng):
        greet(b, lax.rem(g + r, ng))

    small = [pltpu.make_async_copy(s, t, in_sem.at[i]) for i, (s, t) in enumerate(
        ((en_h, en), (bos_h, bos), (fp_h, fp), (fw_h, fw)))]
    local = pltpu.make_async_copy(el, mine, loc_sem.at[0])
    local.start()

    def placed():
        return pltpu.make_async_copy(el, gat.at[:, pl.ds(pl.multiple_of(z * pad, pad), rows), :], loc_sem.at[1])

    @pl.when(straight)
    def _():
        placed().start()

    for copy in small:
        copy.start()

    def slice_of(j):
        ys = 1 - y if j < 2 else y
        xs = x if j % 2 else 1 - x
        return ys * 2 + xs

    def w_copy(j, o):
        w = c if o else 1 - c
        cols = pl.ds(pl.multiple_of(slice_of(j) * depth, depth), depth)
        return pltpu.make_async_copy(wh.at[w, :, :, cols], wv.at[o, j], w_sem.at[o, j])

    order = ((0, 0), (1, 0), (0, 1), (1, 1), (2, 0), (3, 0), (2, 1), (3, 1))
    for j, o in order:
        w_copy(j, o).start()
    local.wait()

    @pl.when(straight)
    def _():
        placed().wait()

    below = jnp.where(z > 0, 1, 0)
    above = jnp.where(z < nz - 1, 1, 0)
    pl.semaphore_wait(barrier, ng + 1 + below + above)

    unit = rows // 6
    pieces = ((0, 2 * unit), (2 * unit, 2 * unit), (4 * unit, unit), (5 * unit, unit))
    parts = range(len(pieces))

    def block(zs, i):
        start, size = pieces[i]
        return gat.at[:, pl.ds(pl.multiple_of(zs * pad + start, unit), size), :]

    def send(zs, i, band, sem):
        ref = block(zs, i)
        return pltpu.make_async_remote_copy(
            src_ref=ref, dst_ref=ref, send_sem=sem, recv_sem=g_recv.at[zs, i], device_id=(band, g), device_id_type=MESH)

    def swap(i):
        start, size = pieces[i]
        return pltpu.make_async_remote_copy(
            src_ref=mine.at[:, pl.ds(start, size), :], dst_ref=block(z, i), send_sem=sw_ss.at[i],
            recv_sem=g_recv.at[z, i], device_id=(xb, mate), device_id_type=MESH)

    def arrived(zs, i):
        send(zs, i, b, up_sem.at[zs, i]).wait_recv()

    def send_z(zs, i, up, down):
        if up:
            @pl.when(z < nz - 1)
            def _():
                send(zs, i, b + NX, up_sem.at[zs, i]).start()

        if down:
            @pl.when(z > 0)
            def _():
                send(zs, i, b - NX, dn_sem.at[zs, i]).start()

    def fwd(s, which=parts):
        for i in which:
            for zs, up in ((z - s, True), (z + s, False)):
                @pl.when((zs >= 0) & (zs < nz))
                def _():
                    arrived(zs, i)
                    send_z(zs, i, up, not up)

    def swapped(which):
        @pl.when(crossed)
        def _():
            for i in which:
                arrived(z, i)
                send_z(z, i, True, True)

    @pl.when(straight)
    def _():
        for i in parts:
            send_z(z, i, True, True)

    @pl.when(crossed)
    def _():
        for i in parts:
            swap(i).start()

    er = mine[0]
    ei = mine[1]
    a_ref[:rows, :depth] = er
    a_ref[:rows, depth:] = ei
    a_ref[rows:, :depth] = -ei
    a_ref[rows:, depth:] = er

    def d_copy(j):
        return pltpu.make_async_remote_copy(
            src_ref=dsend.at[j], dst_ref=drecv.at[j], send_sem=d_ss.at[j], recv_sem=d_rs.at[j],
            device_id=(b, mate), device_id_type=MESH)

    def y_copy(j, h):
        return pltpu.make_async_remote_copy(
            src_ref=ysend.at[j, h], dst_ref=yrecv.at[j, h], send_sem=y_ss.at[j, h], recv_sem=y_rs.at[j, h],
            device_id=(b, across), device_id_type=MESH)

    def x_copy(h):
        return pltpu.make_async_remote_copy(
            src_ref=xsend.at[h], dst_ref=lv.at[x, c, h], send_sem=x_ss.at[h], recv_sem=x_rs.at[h],
            device_id=(xb, g), device_id_type=MESH)

    def l_copy(v, band, h):
        ref = lv.at[band, c, h]
        return pltpu.make_async_remote_copy(
            src_ref=ref, dst_ref=ref, send_sem=l_ss.at[v, h], recv_sem=l_rs.at[v, h],
            device_id=(b, mate), device_id_type=MESH)

    def first(j, o):
        w_copy(j, o).wait()
        part = jnp.dot(a_ref[...], wv[o, j].reshape(2 * depth, depth), preferred_element_type=F32)
        if not o:
            dsend[j] = part.astype(BF16)
            d_copy(j).start()
            return
        d_copy(j).wait_recv()
        part = part + drecv[j].astype(F32)
        for h in range(CUTS):
            if j < 2:
                ysend[j, h] = part[h * cut : (h + 1) * cut].astype(BF16)
                y_copy(j, h).start()
            else:
                held[j - 2, h] = part[h * cut : (h + 1) * cut]

    def to_x(h):
        y_copy(0, h).wait_recv()
        xsend[h] = (held[0, h] + yrecv[0, h].astype(F32)).astype(BF16)
        x_copy(h).start()

    def here(h):
        y_copy(1, h).wait_recv()
        lv[x, c, h] = (held[1, h] + yrecv[1, h].astype(F32)).astype(BF16)
        l_copy(0, x, h).start()

    def from_x(h):
        x_copy(h).wait_recv()
        l_copy(1, 1 - x, h).start()

    def ready():
        for other in range(NX):
            for h in range(CUTS):
                l_copy(other, x, h).wait_recv()
        half = CUTS // 2
        for v in range(NX):
            for w in range(2):
                lw[v, w, :half] = -lv[v, w, half:]
                lw[v, w, half:] = lv[v, w, :half]

    def consume(zs, count):
        at = pl.ds(pl.multiple_of(zs * pad, pad), count * pad)
        pr = lax.dot_general(lv[...].reshape(8 * rows, depth), gat[0, at, :], NT, preferred_element_type=F32)
        pr = pr + lax.dot_general(lw[...].reshape(8 * rows, depth), gat[1, at, :], NT, preferred_element_type=F32)
        for t in range(count):
            scale_and_send(zs + t, pr[:, t * pad : t * pad + rows])

    def scale_and_send(zs, pr):
        k = zs * NX + c
        q, p = k // per, lax.rem(k, per)
        srow = [scr[k, w : w + 1, :] for w in range(2)]
        for v in range(NX):
            f = [cols[v][w] + srow[w] for w in range(2)]
            each = [pr[(4 * v + i) * rows : (4 * v + i + 1) * rows] for i in range(4)]
            total = pack(*[f[0] * each[i] + f[1] * each[2 + i] for i in range(2)])
            home = (q == g) & (x == v)

            @pl.when(home)
            def _():
                own[p] = total
                srecv[x * 2 + y, p] = jnp.zeros(total.shape, BF16)

            @pl.when(jnp.logical_not(home))
            def _():
                ssend[zs, v] = total.astype(BF16)
                pltpu.make_async_remote_copy(
                    src_ref=ssend.at[zs, v], dst_ref=srecv.at[x * 2 + y, p], send_sem=s_ss.at[zs, v],
                    recv_sem=s_rs.at[x * 2 + y, p], device_id=(z * NX + v, q), device_id_type=MESH).start()

    first(0, 0)
    first(1, 0)

    for copy in small:
        copy.wait()
    row = lax.broadcasted_iota(jnp.int32, (16, slots), 0)
    e = en[...].reshape(1, slots)
    hi = e.astype(BF16).astype(F32)
    mid = (e - hi).astype(BF16).astype(F32)
    lo = e - hi - mid
    e3[...] = jnp.where(row == 0, hi, jnp.where(row == 1, mid, jnp.where(row == 2, lo, 0.0))).astype(BF16)
    tile = slots if slots <= 1024 else 8 * rows

    for u in range(slots // tile):
        slot = bos[u * tile : (u + 1) * tile].reshape(1, tile)

        def add(j, acc):
            at = pl.multiple_of(j * tile, tile)
            hit = lax.broadcasted_iota(jnp.int32, (tile, tile), 0) + at == slot
            return acc + jnp.dot(e3[:, pl.ds(at, tile)], jnp.where(hit, 1.0, 0.0).astype(BF16),
                                 preferred_element_type=F32)

        acc = lax.fori_loop(0, slots // tile, add, jnp.zeros((16, tile), F32))
        energy = jnp.sum(acc, axis=0, keepdims=True)
        for w in range(2):
            off = energy - fp[w]
            value = 0.5 * (fw[w] / (1.0 + 4.0 * off * off))
            for v in range(tile // rows):
                scr[u * (tile // rows) + v, w : w + 1, :] = value[:, v * rows : (v + 1) * rows]
    pick = lax.broadcasted_iota(jnp.int32, (rows, rows), 1) == lax.broadcasted_iota(
        jnp.int32, (rows, rows), 0)
    cols = [[jnp.sum(jnp.where(pick, scr[band, w : w + 1, :], 0.0), axis=1, keepdims=True)
             for w in range(2)] for band in (z * NX, z * NX + 1)]

    first(0, 1)
    first(1, 1)
    first(2, 0)
    first(3, 0)
    swapped((0, 1))
    first(2, 1)
    swapped((2, 3))
    first(3, 1)
    own[...] = jnp.zeros(own.shape, F32)

    @pl.when(straight)
    def _():
        fwd(1, (0, 1))
        to_x(0)
        fwd(1, (2, 3))
        to_x(1)
        to_x(2)
        fwd(2, (0,))
        to_x(3)
        fwd(2, (1,))
        here(0)
        from_x(0)
        fwd(2, (2,))
        here(1)
        from_x(1)
        fwd(2, (3,))

    @pl.when(crossed)
    def _():
        to_x(0)
        to_x(1)
        fwd(1, (0, 1))
        to_x(2)
        fwd(1, (2,))
        to_x(3)
        fwd(1, (3,))
        here(0)
        from_x(0)
        fwd(2, (0,))
        here(1)
        from_x(1)
        fwd(2, (1,))

    here(2)
    from_x(2)
    here(3)
    from_x(3)

    @pl.when(crossed)
    def _():
        fwd(2, (2, 3))

    ready()
    consume(z // 2 * 2, 2)

    def tail(t, carry):
        for near, far in ((2 * (z // 2 - t) + 1, 2 * (z // 2 - t)), (2 * (z // 2 + t), 2 * (z // 2 + t) + 1)):
            @pl.when((near >= 0) & (near < nz))
            def _():
                consume(near, 1)

        fwd(2 * t + 1)
        for near, far in ((2 * (z // 2 - t) + 1, 2 * (z // 2 - t)), (2 * (z // 2 + t), 2 * (z // 2 + t) + 1)):
            @pl.when((near >= 0) & (near < nz))
            def _():
                consume(far, 1)

        @pl.when(2 * t + 2 < nz)
        def _():
            fwd(2 * t + 2)

        return carry

    lax.fori_loop(1, nz // 2, tail, 0)

    chip = x * 2 + y
    for p in range(per):
        for r in range(CHIPS):
            @pl.when(jnp.logical_not((chip == r) & (c == p % 2)))
            def _():
                pltpu.make_async_remote_copy(
                    src_ref=ssend.at[0, 0], dst_ref=srecv.at[r, p], send_sem=s_ss.at[0, 0], recv_sem=s_rs.at[r, p],
                    device_id=(b, mate), device_id_type=MESH).wait_recv()
        total = own[p]
        for r in range(CHIPS):
            total = total + srecv[r, p].astype(F32)
        for i, each in enumerate(unpack(total, rows)):
            out[i, :, p * rows : (p + 1) * rows] = each

    def sent(zs, carry):
        for i in parts:
            @pl.when((zs <= z) & (z < nz - 1))
            def _():
                send(zs, i, b, up_sem.at[zs, i]).wait_send()

            @pl.when((zs >= z) & (z > 0))
            def _():
                send(zs, i, b, dn_sem.at[zs, i]).wait_send()

        q = (zs * NX + c) // per
        for v in range(NX):
            @pl.when((q != g) | (x != v))
            def _():
                pltpu.make_async_remote_copy(
                    src_ref=ssend.at[zs, v], dst_ref=srecv.at[0, 0], send_sem=s_ss.at[zs, v], recv_sem=s_rs.at[0, 0],
                    device_id=(b, mate), device_id_type=MESH).wait_send()

        return carry

    lax.fori_loop(0, nz, sent, 0)

    @pl.when(crossed)
    def _():
        for i in parts:
            swap(i).wait_send()

    for j in range(4):
        d_copy(j).wait_send()
    for h in range(CUTS):
        for j in range(2):
            y_copy(j, h).wait_send()
            l_copy(j, x, h).wait_send()
        x_copy(h).wait_send()


def solution(mesh):
    nb, ng = mesh.shape["band"], mesh.shape["ga"]
    nz = nb // NX
    per = nb // ng

    def step(elements, screened, energies, freq_points, freq_weights, band_of_slot):
        _, rows, depth = elements.shape
        slots = energies.shape[0]
        pad = -(-rows // 128) * 128
        cut = 2 * rows // CUTS
        packed = (3 * rows // 2, LANES) if packs(rows) else (2 * rows, rows)
        any_space = pl.BlockSpec(memory_space=pl.ANY)
        vmem = pl.BlockSpec(memory_space=pltpu.VMEM)
        dma = pltpu.SemaphoreType.DMA
        return pl.pallas_call(
            functools.partial(kernel, nb, ng),
            out_shape=pltpu.VMEM((2, rows, per * rows), F32),
            in_specs=[any_space] * 6,
            out_specs=vmem,
            scratch_shapes=[
                pltpu.VMEM((slots,), F32), pltpu.VMEM((slots,), jnp.int32),
                pltpu.SMEM(freq_points.shape, F32), pltpu.SMEM(freq_weights.shape, F32),
                pltpu.VMEM((2, rows, depth), BF16),
                pltpu.VMEM((2, nz * pad, depth), BF16),
                pltpu.VMEM((2, 4, 2, depth, depth), BF16),
                pltpu.VMEM((2 * rows, 2 * depth), BF16),
                pltpu.VMEM((16, slots), BF16),
                pltpu.VMEM((nb, 2, rows), F32),
                pltpu.VMEM((2, CUTS, cut, depth), F32),
                pltpu.VMEM((4, 2 * rows, depth), BF16),
                pltpu.VMEM((4, 2 * rows, depth), BF16),
                pltpu.VMEM((2, CUTS, cut, depth), BF16),
                pltpu.VMEM((2, CUTS, cut, depth), BF16),
                pltpu.VMEM((CUTS, cut, depth), BF16),
                pltpu.VMEM((NX, 2, CUTS, cut, depth), BF16),
                pltpu.VMEM((NX, 2, CUTS, cut, depth), BF16),
                pltpu.VMEM((nz, NX) + packed, BF16),
                pltpu.VMEM((CHIPS, per) + packed, BF16),
                pltpu.VMEM((per,) + packed, F32),
                dma((4,)), dma((2,)), dma((2, 4)), dma((4,)), dma((nz, 4)), dma((nz, 4)), dma((nz, 4)),
                dma((4,)), dma((4,)), dma((2, CUTS)), dma((2, CUTS)), dma((CUTS,)), dma((CUTS,)), dma((2, CUTS)), dma((2, CUTS)),
                dma((nz, NX)), dma((CHIPS, per)),
            ],
            compiler_params=pltpu.CompilerParams(
                collective_id=0, has_side_effects=True, vmem_limit_bytes=60 * 1024 * 1024),
        )(elements, screened, energies, band_of_slot, freq_points, freq_weights)

    placed = (P(None, "band", "ga"), P(None, None, "ga", None), P(), P(), P(), P())
    return jax.shard_map(
        step, mesh=mesh, in_specs=placed, out_specs=P(None, "band", "ga"), check_vma=False
    )
```

```python
import functools

import jax
import jax.numpy as jnp
from jax import lax
from jax.experimental import pallas as pl
from jax.experimental.pallas import tpu as pltpu
from jax.sharding import PartitionSpec as P

MESH = pl.DeviceIdType.MESH
F32 = jnp.float32
BF16 = jnp.bfloat16
NT = (((1,), (1,)), ((), ()))
NX = 2
CUTS = 4
LANES = 128
CHIPS = 4


def packs(rows):
    return 2 * (2 * rows - LANES) == LANES


def pack(re, im):
    rows = re.shape[0]
    if not packs(rows):
        return jnp.concatenate([re, im], axis=0)
    spare = LANES - rows
    top = jnp.concatenate([re, im[:, :spare]], axis=1)
    rest = im[:, spare:]
    return jnp.concatenate([top, jnp.concatenate([rest[: rows // 2], rest[rows // 2 :]], axis=1)], axis=0)


def unpack(both, rows):
    if not packs(rows):
        return both[:rows], both[rows:]
    rest = both[rows:]
    rest = jnp.concatenate([rest[:, : LANES // 2], rest[:, LANES // 2 :]], axis=0)
    return both[:rows, :rows], jnp.concatenate([both[:rows, rows:], rest], axis=1)


def kernel(nb, ng, el, wh, en_h, bos_h, fp_h, fw_h, out, *scratch):
    (en, bos, fp, fw, mine, gat, wv, a_ref, e3, scr, held, dsend, drecv, ysend, yrecv, xsend, lv, lw, ssend, srecv, own,
     in_sem, loc_sem, w_sem, sw_ss, up_sem, dn_sem, g_recv, d_ss, d_rs, y_ss, y_rs, x_ss, x_rs, l_ss, l_rs, s_ss,
     s_rs) = scratch
    rows, depth = el.shape[1], el.shape[2]
    nz = nb // NX
    pad = gat.shape[1] // nz
    cut = 2 * rows // CUTS
    per = nb // ng
    slots = en.shape[0]
    b, g = lax.axis_index("band"), lax.axis_index("ga")
    z, x = b // NX, lax.rem(b, NX)
    y, c = g // 2, lax.rem(g, 2)
    mate = g + 1 - 2 * c
    across = lax.rem(g + 2, ng)
    xb = b + 1 - 2 * x
    straight = x == c
    crossed = x != c

    barrier = pltpu.get_barrier_semaphore()

    def greet(band, ga):
        pl.semaphore_signal(barrier, inc=1, device_id=(band, ga), device_id_type=MESH)

    @pl.when(z > 0)
    def _():
        greet(b - NX, g)

    @pl.when(z < nz - 1)
    def _():
        greet(b + NX, g)

    greet(xb, g)
    greet(xb, mate)
    for r in range(1, ng):
        greet(b, lax.rem(g + r, ng))

    small = [pltpu.make_async_copy(s, t, in_sem.at[i]) for i, (s, t) in enumerate(
        ((en_h, en), (bos_h, bos), (fp_h, fp), (fw_h, fw)))]
    local = pltpu.make_async_copy(el, mine, loc_sem.at[0])
    local.start()

    def placed():
        return pltpu.make_async_copy(el, gat.at[:, pl.ds(pl.multiple_of(z * pad, pad), rows), :], loc_sem.at[1])

    @pl.when(straight)
    def _():
        placed().start()

    for copy in small:
        copy.start()

    def slice_of(j):
        ys = lax.rem(y + 1 - j // 2, 2)
        xs = lax.rem(x + 1 + j, 2)
        return ys * 2 + xs

    def w_copy(j, o):
        w = c if o else 1 - c
        cols = pl.ds(pl.multiple_of(slice_of(j) * depth, depth), depth)
        return pltpu.make_async_copy(wh.at[w, :, :, cols], wv.at[o, j], w_sem.at[o, j])

    def load(j, carry):
        for o in range(2):
            w_copy(j, o).start()
        return carry

    lax.fori_loop(0, 4, load, 0)
    local.wait()

    @pl.when(straight)
    def _():
        placed().wait()

    below = jnp.where(z > 0, 1, 0)
    above = jnp.where(z < nz - 1, 1, 0)
    pl.semaphore_wait(barrier, ng + 1 + below + above)

    unit = rows // 6
    pieces = ((0, 2 * unit), (2 * unit, 2 * unit), (4 * unit, unit), (5 * unit, unit))
    parts = range(len(pieces))

    def block(zs, i):
        start, size = pieces[i]
        return gat.at[:, pl.ds(pl.multiple_of(zs * pad + start, unit), size), :]

    def send(zs, i, band, sem):
        ref = block(zs, i)
        return pltpu.make_async_remote_copy(
            src_ref=ref, dst_ref=ref, send_sem=sem, recv_sem=g_recv.at[zs, i], device_id=(band, g), device_id_type=MESH)

    def swap(i):
        start, size = pieces[i]
        return pltpu.make_async_remote_copy(
            src_ref=mine.at[:, pl.ds(start, size), :], dst_ref=block(z, i), send_sem=sw_ss.at[i],
            recv_sem=g_recv.at[z, i], device_id=(xb, mate), device_id_type=MESH)

    def arrived(zs, i):
        send(zs, i, b, up_sem.at[zs, i]).wait_recv()

    def send_z(zs, i, up, down):
        if up:
            @pl.when(z < nz - 1)
            def _():
                send(zs, i, b + NX, up_sem.at[zs, i]).start()

        if down:
            @pl.when(z > 0)
            def _():
                send(zs, i, b - NX, dn_sem.at[zs, i]).start()

    def fwd(s, which=parts):
        for i in which:
            for zs, up in ((z - s, True), (z + s, False)):
                @pl.when((zs >= 0) & (zs < nz))
                def _():
                    arrived(zs, i)
                    send_z(zs, i, up, not up)

    def swapped(which):
        @pl.when(crossed)
        def _():
            for i in which:
                arrived(z, i)
                send_z(z, i, True, True)

    @pl.when(straight)
    def _():
        for i in parts:
            send_z(z, i, True, True)

    @pl.when(crossed)
    def _():
        for i in parts:
            swap(i).start()

    er = mine[0]
    ei = mine[1]
    a_ref[:rows, :depth] = er
    a_ref[:rows, depth:] = ei
    a_ref[rows:, :depth] = -ei
    a_ref[rows:, depth:] = er

    def d_copy(j):
        return pltpu.make_async_remote_copy(
            src_ref=dsend.at[j], dst_ref=drecv.at[j], send_sem=d_ss.at[j], recv_sem=d_rs.at[j],
            device_id=(b, mate), device_id_type=MESH)

    def y_copy(j, h):
        return pltpu.make_async_remote_copy(
            src_ref=ysend.at[j, h], dst_ref=yrecv.at[j, h], send_sem=y_ss.at[j, h], recv_sem=y_rs.at[j, h],
            device_id=(b, across), device_id_type=MESH)

    def x_copy(h):
        return pltpu.make_async_remote_copy(
            src_ref=xsend.at[h], dst_ref=lv.at[x, c, h], send_sem=x_ss.at[h], recv_sem=x_rs.at[h],
            device_id=(xb, g), device_id_type=MESH)

    def l_copy(v, band, h):
        ref = lv.at[band, c, h]
        return pltpu.make_async_remote_copy(
            src_ref=ref, dst_ref=ref, send_sem=l_ss.at[v, h], recv_sem=l_rs.at[v, h],
            device_id=(b, mate), device_id_type=MESH)

    def first(j, o):
        w_copy(j, o).wait()
        part = jnp.dot(a_ref[...], wv[o, j].reshape(2 * depth, depth), preferred_element_type=F32)
        if not o:
            dsend[j] = part.astype(BF16)
            d_copy(j).start()
            return
        d_copy(j).wait_recv()
        part = part + drecv[j].astype(F32)
        for h in range(CUTS):
            if j < 2:
                ysend[j, h] = part[h * cut : (h + 1) * cut].astype(BF16)
                y_copy(j, h).start()
            else:
                held[j - 2, h] = part[h * cut : (h + 1) * cut]

    def to_x(h):
        y_copy(0, h).wait_recv()
        xsend[h] = (held[0, h] + yrecv[0, h].astype(F32)).astype(BF16)
        x_copy(h).start()

    def here(h):
        y_copy(1, h).wait_recv()
        lv[x, c, h] = (held[1, h] + yrecv[1, h].astype(F32)).astype(BF16)
        l_copy(0, x, h).start()

    def from_x(h):
        x_copy(h).wait_recv()
        l_copy(1, 1 - x, h).start()

    def ready():
        for other in range(NX):
            for h in range(CUTS):
                l_copy(other, x, h).wait_recv()
        half = CUTS // 2
        for v in range(NX):
            for w in range(2):
                lw[v, w, :half] = -lv[v, w, half:]
                lw[v, w, half:] = lv[v, w, :half]

    def consume(zs, count):
        at = pl.ds(pl.multiple_of(zs * pad, pad), count * pad)
        pr = lax.dot_general(lv[...].reshape(8 * rows, depth), gat[0, at, :], NT, preferred_element_type=F32)
        pr = pr + lax.dot_general(lw[...].reshape(8 * rows, depth), gat[1, at, :], NT, preferred_element_type=F32)
        for t in range(count):
            scale_and_send(zs + t, pr[:, t * pad : t * pad + rows])

    def scale_and_send(zs, pr):
        k = zs * NX + c
        q, p = k // per, lax.rem(k, per)
        srow = [scr[k, w : w + 1, :] for w in range(2)]
        for v in range(NX):
            f = [cols[v][w] + srow[w] for w in range(2)]
            each = [pr[(4 * v + i) * rows : (4 * v + i + 1) * rows] for i in range(4)]
            total = pack(*[f[0] * each[i] + f[1] * each[2 + i] for i in range(2)])
            home = (q == g) & (x == v)

            @pl.when(home)
            def _():
                own[p] = total
                srecv[x * 2 + y, p] = jnp.zeros(total.shape, BF16)

            @pl.when(jnp.logical_not(home))
            def _():
                ssend[zs, v] = total.astype(BF16)
                pltpu.make_async_remote_copy(
                    src_ref=ssend.at[zs, v], dst_ref=srecv.at[x * 2 + y, p], send_sem=s_ss.at[zs, v],
                    recv_sem=s_rs.at[x * 2 + y, p], device_id=(z * NX + v, q), device_id_type=MESH).start()

    first(0, 0)
    first(1, 0)

    for copy in small:
        copy.wait()
    row = lax.broadcasted_iota(jnp.int32, (16, slots), 0)
    e = en[...].reshape(1, slots)
    hi = e.astype(BF16).astype(F32)
    mid = (e - hi).astype(BF16).astype(F32)
    lo = e - hi - mid
    e3[...] = jnp.where(row == 0, hi, jnp.where(row == 1, mid, jnp.where(row == 2, lo, 0.0))).astype(BF16)
    tile = slots if slots <= 1024 else 8 * rows

    for u in range(slots // tile):
        slot = bos[u * tile : (u + 1) * tile].reshape(1, tile)

        def add(j, acc):
            at = pl.multiple_of(j * tile, tile)
            hit = lax.broadcasted_iota(jnp.int32, (tile, tile), 0) + at == slot
            return acc + jnp.dot(e3[:, pl.ds(at, tile)], jnp.where(hit, 1.0, 0.0).astype(BF16),
                                 preferred_element_type=F32)

        acc = lax.fori_loop(0, slots // tile, add, jnp.zeros((16, tile), F32))
        energy = jnp.sum(acc, axis=0, keepdims=True)
        for w in range(2):
            off = energy - fp[w]
            value = 0.5 * (fw[w] / (1.0 + 4.0 * off * off))
            for v in range(tile // rows):
                scr[u * (tile // rows) + v, w : w + 1, :] = value[:, v * rows : (v + 1) * rows]
    pick = lax.broadcasted_iota(jnp.int32, (rows, rows), 1) == lax.broadcasted_iota(
        jnp.int32, (rows, rows), 0)
    cols = [[jnp.sum(jnp.where(pick, scr[band, w : w + 1, :], 0.0), axis=1, keepdims=True)
             for w in range(2)] for band in (z * NX, z * NX + 1)]

    first(0, 1)
    first(1, 1)
    first(2, 0)
    first(3, 0)
    swapped((0, 1))
    first(2, 1)
    swapped((2, 3))
    first(3, 1)
    own[...] = jnp.zeros(own.shape, F32)

    @pl.when(straight)
    def _():
        fwd(1, (0, 1))
        to_x(0)
        fwd(1, (2, 3))
        to_x(1)
        to_x(2)
        fwd(2, (0,))
        to_x(3)
        fwd(2, (1,))
        here(0)
        from_x(0)
        fwd(2, (2,))
        here(1)
        from_x(1)
        fwd(2, (3,))

    @pl.when(crossed)
    def _():
        to_x(0)
        to_x(1)
        fwd(1, (0, 1))
        to_x(2)
        fwd(1, (2,))
        to_x(3)
        fwd(1, (3,))
        here(0)
        from_x(0)
        fwd(2, (0,))
        here(1)
        from_x(1)
        fwd(2, (1,))

    here(2)
    from_x(2)
    here(3)
    from_x(3)

    @pl.when(crossed)
    def _():
        fwd(2, (2, 3))

    ready()
    consume(z // 2 * 2, 2)

    def tail(t, carry):
        for near, far in ((2 * (z // 2 - t) + 1, 2 * (z // 2 - t)), (2 * (z // 2 + t), 2 * (z // 2 + t) + 1)):
            @pl.when((near >= 0) & (near < nz))
            def _():
                consume(near, 1)

        fwd(2 * t + 1)
        for near, far in ((2 * (z // 2 - t) + 1, 2 * (z // 2 - t)), (2 * (z // 2 + t), 2 * (z // 2 + t) + 1)):
            @pl.when((near >= 0) & (near < nz))
            def _():
                consume(far, 1)

        @pl.when(2 * t + 2 < nz)
        def _():
            fwd(2 * t + 2)

        return carry

    lax.fori_loop(1, nz // 2, tail, 0)

    chip = x * 2 + y
    for p in range(per):
        for r in range(CHIPS):
            @pl.when(jnp.logical_not((chip == r) & (c == p % 2)))
            def _():
                pltpu.make_async_remote_copy(
                    src_ref=ssend.at[0, 0], dst_ref=srecv.at[r, p], send_sem=s_ss.at[0, 0], recv_sem=s_rs.at[r, p],
                    device_id=(b, mate), device_id_type=MESH).wait_recv()
        total = own[p]
        for r in range(CHIPS):
            total = total + srecv[r, p].astype(F32)
        for i, each in enumerate(unpack(total, rows)):
            out[i, :, p * rows : (p + 1) * rows] = each

    def sent(zs, carry):
        for i in parts:
            @pl.when((zs <= z) & (z < nz - 1))
            def _():
                send(zs, i, b, up_sem.at[zs, i]).wait_send()

            @pl.when((zs >= z) & (z > 0))
            def _():
                send(zs, i, b, dn_sem.at[zs, i]).wait_send()

        q = (zs * NX + c) // per
        for v in range(NX):
            @pl.when((q != g) | (x != v))
            def _():
                pltpu.make_async_remote_copy(
                    src_ref=ssend.at[zs, v], dst_ref=srecv.at[0, 0], send_sem=s_ss.at[zs, v], recv_sem=s_rs.at[0, 0],
                    device_id=(b, mate), device_id_type=MESH).wait_send()

        return carry

    lax.fori_loop(0, nz, sent, 0)

    @pl.when(crossed)
    def _():
        for i in parts:
            swap(i).wait_send()

    for j in range(4):
        d_copy(j).wait_send()
    for h in range(CUTS):
        for j in range(2):
            y_copy(j, h).wait_send()
            l_copy(j, x, h).wait_send()
        x_copy(h).wait_send()


def solution(mesh):
    nb, ng = mesh.shape["band"], mesh.shape["ga"]
    nz = nb // NX
    per = nb // ng

    def step(elements, screened, energies, freq_points, freq_weights, band_of_slot):
        _, rows, depth = elements.shape
        slots = energies.shape[0]
        pad = -(-rows // 128) * 128
        cut = 2 * rows // CUTS
        packed = (3 * rows // 2, LANES) if packs(rows) else (2 * rows, rows)
        any_space = pl.BlockSpec(memory_space=pl.ANY)
        vmem = pl.BlockSpec(memory_space=pltpu.VMEM)
        dma = pltpu.SemaphoreType.DMA
        return pl.pallas_call(
            functools.partial(kernel, nb, ng),
            out_shape=pltpu.VMEM((2, rows, per * rows), F32),
            in_specs=[any_space] * 6,
            out_specs=vmem,
            scratch_shapes=[
                pltpu.VMEM((slots,), F32), pltpu.VMEM((slots,), jnp.int32),
                pltpu.SMEM(freq_points.shape, F32), pltpu.SMEM(freq_weights.shape, F32),
                pltpu.VMEM((2, rows, depth), BF16),
                pltpu.VMEM((2, nz * pad, depth), BF16),
                pltpu.VMEM((2, 4, 2, depth, depth), BF16),
                pltpu.VMEM((2 * rows, 2 * depth), BF16),
                pltpu.VMEM((16, slots), BF16),
                pltpu.VMEM((nb, 2, rows), F32),
                pltpu.VMEM((2, CUTS, cut, depth), F32),
                pltpu.VMEM((4, 2 * rows, depth), BF16),
                pltpu.VMEM((4, 2 * rows, depth), BF16),
                pltpu.VMEM((2, CUTS, cut, depth), BF16),
                pltpu.VMEM((2, CUTS, cut, depth), BF16),
                pltpu.VMEM((CUTS, cut, depth), BF16),
                pltpu.VMEM((NX, 2, CUTS, cut, depth), BF16),
                pltpu.VMEM((NX, 2, CUTS, cut, depth), BF16),
                pltpu.VMEM((nz, NX) + packed, BF16),
                pltpu.VMEM((CHIPS, per) + packed, BF16),
                pltpu.VMEM((per,) + packed, F32),
                dma((4,)), dma((2,)), dma((2, 4)), dma((4,)), dma((nz, 4)), dma((nz, 4)), dma((nz, 4)),
                dma((4,)), dma((4,)), dma((2, CUTS)), dma((2, CUTS)), dma((CUTS,)), dma((CUTS,)), dma((2, CUTS)), dma((2, CUTS)),
                dma((nz, NX)), dma((CHIPS, per)),
            ],
            compiler_params=pltpu.CompilerParams(
                collective_id=0, has_side_effects=True, vmem_limit_bytes=60 * 1024 * 1024),
        )(elements, screened, energies, band_of_slot, freq_points, freq_weights)

    placed = (P(None, "band", "ga"), P(None, None, "ga", None), P(), P(), P(), P())
    return jax.shard_map(
        step, mesh=mesh, in_specs=placed, out_specs=P(None, "band", "ga"), check_vma=False
    )
```

```python
import functools

import jax
import jax.numpy as jnp
from jax import lax
from jax.experimental import pallas as pl
from jax.experimental.pallas import tpu as pltpu
from jax.sharding import PartitionSpec as P

MESH = pl.DeviceIdType.MESH
F32 = jnp.float32
BF16 = jnp.bfloat16
NT = (((1,), (1,)), ((), ()))
NX = 2
CUTS = 4
LANES = 128
CHIPS = 4


def packs(rows):
    return 2 * (2 * rows - LANES) == LANES


def pack(re, im):
    rows = re.shape[0]
    if not packs(rows):
        return jnp.concatenate([re, im], axis=0)
    spare = LANES - rows
    top = jnp.concatenate([re, im[:, :spare]], axis=1)
    rest = im[:, spare:]
    return jnp.concatenate([top, jnp.concatenate([rest[: rows // 2], rest[rows // 2 :]], axis=1)], axis=0)


def unpack(both, rows):
    if not packs(rows):
        return both[:rows], both[rows:]
    rest = both[rows:]
    rest = jnp.concatenate([rest[:, : LANES // 2], rest[:, LANES // 2 :]], axis=0)
    return both[:rows, :rows], jnp.concatenate([both[:rows, rows:], rest], axis=1)


def kernel(nb, ng, el, wh, en_h, bos_h, fp_h, fw_h, out, *scratch):
    (en, bos, fp, fw, mine, gat, wv, a_ref, e3, scr, held, dsend, drecv, ysend, yrecv, xsend, lv, lw, ssend, srecv, own,
     in_sem, loc_sem, w_sem, sw_ss, up_sem, dn_sem, g_recv, d_ss, d_rs, y_ss, y_rs, x_ss, x_rs, l_ss, l_rs, s_ss,
     s_rs) = scratch
    rows, depth = el.shape[1], el.shape[2]
    nz = nb // NX
    pad = gat.shape[1] // nz
    cut = 2 * rows // CUTS
    per = nb // ng
    slots = en.shape[0]
    b, g = lax.axis_index("band"), lax.axis_index("ga")
    z, x = b // NX, lax.rem(b, NX)
    y, c = g // 2, lax.rem(g, 2)
    mate = g + 1 - 2 * c
    across = lax.rem(g + 2, ng)
    xb = b + 1 - 2 * x
    straight = x == c
    crossed = x != c

    barrier = pltpu.get_barrier_semaphore()

    def greet(band, ga):
        pl.semaphore_signal(barrier, inc=1, device_id=(band, ga), device_id_type=MESH)

    @pl.when(z > 0)
    def _():
        greet(b - NX, g)

    @pl.when(z < nz - 1)
    def _():
        greet(b + NX, g)

    greet(xb, g)
    greet(xb, mate)
    for r in range(1, ng):
        greet(b, lax.rem(g + r, ng))

    small = [pltpu.make_async_copy(s, t, in_sem.at[i]) for i, (s, t) in enumerate(
        ((en_h, en), (bos_h, bos), (fp_h, fp), (fw_h, fw)))]
    local = pltpu.make_async_copy(el, mine, loc_sem.at[0])
    local.start()

    def placed():
        return pltpu.make_async_copy(el, gat.at[:, pl.ds(pl.multiple_of(z * pad, pad), rows), :], loc_sem.at[1])

    @pl.when(straight)
    def _():
        placed().start()

    for copy in small:
        copy.start()

    def slice_of(j):
        ys = lax.rem(y + 1 - j // 2, 2)
        xs = lax.rem(x + 1 + j, 2)
        return ys * 2 + xs

    def w_copy(j, o):
        w = c if o else 1 - c
        cols = pl.ds(pl.multiple_of(slice_of(j) * depth, depth), depth)
        return pltpu.make_async_copy(wh.at[w, :, :, cols], wv.at[o, j], w_sem.at[o, j])

    def load(j, carry):
        for o in range(2):
            w_copy(j, o).start()
        return carry

    lax.fori_loop(0, 4, load, 0)
    local.wait()

    @pl.when(straight)
    def _():
        placed().wait()

    below = jnp.where(z > 0, 1, 0)
    above = jnp.where(z < nz - 1, 1, 0)
    pl.semaphore_wait(barrier, ng + 1 + below + above)

    unit = rows // 6
    pieces = ((0, 2 * unit), (2 * unit, 2 * unit), (4 * unit, unit), (5 * unit, unit))
    parts = range(len(pieces))

    def block(zs, i):
        start, size = pieces[i]
        return gat.at[:, pl.ds(pl.multiple_of(zs * pad + start, unit), size), :]

    def send(zs, i, band, sem):
        ref = block(zs, i)
        return pltpu.make_async_remote_copy(
            src_ref=ref, dst_ref=ref, send_sem=sem, recv_sem=g_recv.at[zs, i], device_id=(band, g), device_id_type=MESH)

    def swap(i):
        start, size = pieces[i]
        return pltpu.make_async_remote_copy(
            src_ref=mine.at[:, pl.ds(start, size), :], dst_ref=block(z, i), send_sem=sw_ss.at[i],
            recv_sem=g_recv.at[z, i], device_id=(xb, mate), device_id_type=MESH)

    def arrived(zs, i):
        send(zs, i, b, up_sem.at[zs, i]).wait_recv()

    def send_z(zs, i, up, down):
        if up:
            @pl.when(z < nz - 1)
            def _():
                send(zs, i, b + NX, up_sem.at[zs, i]).start()

        if down:
            @pl.when(z > 0)
            def _():
                send(zs, i, b - NX, dn_sem.at[zs, i]).start()

    def fwd(s, which=parts, ways=(True, False)):
        for i in which:
            for up in ways:
                zs = z - s if up else z + s

                @pl.when((zs >= 0) & (zs < nz))
                def _():
                    arrived(zs, i)
                    send_z(zs, i, up, not up)

    def swapped(which):
        @pl.when(crossed)
        def _():
            for i in which:
                arrived(z, i)
                send_z(z, i, True, True)

    def early(which):
        @pl.when(straight)
        def _():
            fwd(1, which, (True,))

    @pl.when(straight)
    def _():
        for i in parts:
            send_z(z, i, True, True)

    @pl.when(crossed)
    def _():
        for i in parts:
            swap(i).start()

    er = mine[0]
    ei = mine[1]
    a_ref[:rows, :depth] = er
    a_ref[:rows, depth:] = ei
    a_ref[rows:, :depth] = -ei
    a_ref[rows:, depth:] = er

    def d_copy(j):
        return pltpu.make_async_remote_copy(
            src_ref=dsend.at[j], dst_ref=drecv.at[j], send_sem=d_ss.at[j], recv_sem=d_rs.at[j],
            device_id=(b, mate), device_id_type=MESH)

    def y_copy(j, h):
        return pltpu.make_async_remote_copy(
            src_ref=ysend.at[j, h], dst_ref=yrecv.at[j, h], send_sem=y_ss.at[j, h], recv_sem=y_rs.at[j, h],
            device_id=(b, across), device_id_type=MESH)

    def x_copy(h):
        return pltpu.make_async_remote_copy(
            src_ref=xsend.at[h], dst_ref=lv.at[x, c, h], send_sem=x_ss.at[h], recv_sem=x_rs.at[h],
            device_id=(xb, g), device_id_type=MESH)

    def l_copy(v, band, h):
        ref = lv.at[band, c, h]
        return pltpu.make_async_remote_copy(
            src_ref=ref, dst_ref=ref, send_sem=l_ss.at[v, h], recv_sem=l_rs.at[v, h],
            device_id=(b, mate), device_id_type=MESH)

    def first(j, o):
        w_copy(j, o).wait()
        part = jnp.dot(a_ref[...], wv[o, j].reshape(2 * depth, depth), preferred_element_type=F32)
        if not o:
            dsend[j] = part.astype(BF16)
            d_copy(j).start()
            return
        d_copy(j).wait_recv()
        part = part + drecv[j].astype(F32)
        for h in range(CUTS):
            if j < 2:
                ysend[j, h] = part[h * cut : (h + 1) * cut].astype(BF16)
                y_copy(j, h).start()
            else:
                held[j - 2, h] = part[h * cut : (h + 1) * cut]

    def to_x(h):
        y_copy(0, h).wait_recv()
        xsend[h] = (held[0, h] + yrecv[0, h].astype(F32)).astype(BF16)
        x_copy(h).start()

    def here(h):
        y_copy(1, h).wait_recv()
        lv[x, c, h] = (held[1, h] + yrecv[1, h].astype(F32)).astype(BF16)
        l_copy(0, x, h).start()

    def from_x(h):
        x_copy(h).wait_recv()
        l_copy(1, 1 - x, h).start()

    def ready(other):
        half = CUTS // 2
        v = 1 - x if other else x
        for h in range(CUTS):
            l_copy(other, x, h).wait_recv()
        for w in range(2):
            lw[v, w, :half] = -lv[v, w, half:]
            lw[v, w, half:] = lv[v, w, :half]

    def consume(zs, count, v=None):
        at = pl.ds(pl.multiple_of(zs * pad, pad), count * pad)
        bands = range(NX) if v is None else (v,)
        left, right = [ref[...] if v is None else ref[v] for ref in (lv, lw)]
        shape = (4 * len(bands) * rows, depth)
        pr = lax.dot_general(left.reshape(shape), gat[0, at, :], NT, preferred_element_type=F32)
        pr = pr + lax.dot_general(right.reshape(shape), gat[1, at, :], NT, preferred_element_type=F32)
        for t in range(count):
            for n, band in enumerate(bands):
                scale_and_send(zs + t, band, [
                    pr[(4 * n + i) * rows : (4 * n + i + 1) * rows, t * pad : t * pad + rows] for i in range(4)])

    def scale_and_send(zs, v, each):
        k = zs * NX + c
        q, p = k // per, lax.rem(k, per)
        col = [jnp.where(v == 0, cols[0][w], cols[1][w]) for w in range(2)]
        f = [col[w] + scr[k, w : w + 1, :] for w in range(2)]
        total = [f[0] * each[i] + f[1] * each[2 + i] for i in range(2)]
        home = (q == g) & (x == v)

        @pl.when(home)
        def _():
            own[p] = pack(*total)
            srecv[x * 2 + y, p] = jnp.zeros(srecv.shape[2:], BF16)

        @pl.when(jnp.logical_not(home))
        def _():
            ssend[zs, v] = pack(*[part.astype(BF16) for part in total])
            pltpu.make_async_remote_copy(
                src_ref=ssend.at[zs, v], dst_ref=srecv.at[x * 2 + y, p], send_sem=s_ss.at[zs, v],
                recv_sem=s_rs.at[x * 2 + y, p], device_id=(z * NX + v, q), device_id_type=MESH).start()

    first(0, 0)
    first(1, 0)

    for copy in small:
        copy.wait()
    row = lax.broadcasted_iota(jnp.int32, (16, slots), 0)
    e = en[...].reshape(1, slots)
    hi = e.astype(BF16).astype(F32)
    mid = (e - hi).astype(BF16).astype(F32)
    lo = e - hi - mid
    e3[...] = jnp.where(row == 0, hi, jnp.where(row == 1, mid, jnp.where(row == 2, lo, 0.0))).astype(BF16)
    tile = slots if slots <= 1024 else 8 * rows

    for u in range(slots // tile):
        slot = bos[u * tile : (u + 1) * tile].reshape(1, tile)

        def add(j, acc):
            at = pl.multiple_of(j * tile, tile)
            hit = lax.broadcasted_iota(jnp.int32, (tile, tile), 0) + at == slot
            return acc + jnp.dot(e3[:, pl.ds(at, tile)], jnp.where(hit, 1.0, 0.0).astype(BF16),
                                 preferred_element_type=F32)

        acc = lax.fori_loop(0, slots // tile, add, jnp.zeros((16, tile), F32))
        energy = jnp.sum(acc, axis=0, keepdims=True)
        for w in range(2):
            off = energy - fp[w]
            value = 0.5 * (fw[w] / (1.0 + 4.0 * off * off))
            for v in range(tile // rows):
                scr[u * (tile // rows) + v, w : w + 1, :] = value[:, v * rows : (v + 1) * rows]
    pick = lax.broadcasted_iota(jnp.int32, (rows, rows), 1) == lax.broadcasted_iota(
        jnp.int32, (rows, rows), 0)
    cols = [[jnp.sum(jnp.where(pick, scr[band, w : w + 1, :], 0.0), axis=1, keepdims=True)
             for w in range(2)] for band in (z * NX, z * NX + 1)]

    first(0, 1)
    first(1, 1)
    first(2, 0)
    swapped((0,))
    first(3, 0)
    swapped((1, 2, 3))
    early((0, 1))
    first(2, 1)
    first(3, 1)
    own[...] = jnp.zeros(own.shape, F32)

    @pl.when(straight)
    def _():
        fwd(1, (0, 1), (False,))
        to_x(0)
        fwd(1, (2, 3))
        to_x(1)
        to_x(2)
        to_x(3)
        fwd(2, (0, 1))
        here(0)
        from_x(0)
        fwd(2, (2,))
        here(1)
        from_x(1)
        fwd(2, (3,))

    @pl.when(crossed)
    def _():
        to_x(0)
        to_x(1)
        fwd(1, (0, 1))
        to_x(2)
        fwd(1, (2,))
        to_x(3)
        fwd(1, (3,))
        here(0)
        from_x(0)
        here(1)
        from_x(1)

    even = lax.rem(z, 2) == 0
    edge = (z == 0) | (z == nz - 1)

    @pl.when(crossed & jnp.logical_not(edge))
    def _():
        fwd(2, (0, 1))

    from_x(2)
    from_x(3)
    here(2)

    @pl.when(crossed & jnp.logical_not(edge))
    def _():
        fwd(2, (2, 3))

    here(3)

    for other in (1, 0):
        ready(other)
        v = 1 - x if other else x

        @pl.when(even & (z > 0))
        def _():
            consume(z - 2, 2, v)

        consume(z // 2 * 2, 2, v)

        @pl.when(jnp.logical_not(even) & (z < nz - 1))
        def _():
            consume(z + 1, 2, v)

    @pl.when(crossed & edge)
    def _():
        fwd(2)

    def tail(t, carry):
        base = z // 2 * 2
        inner = base + jnp.where(even, -2 * t, 2 * t)
        near = jnp.where(even, base + 2 * t, base - 2 * t + 1)
        far = jnp.where(even, near + 1, near - 1)

        @pl.when((t > 1) & (inner >= 0) & (inner < nz))
        def _():
            consume(inner, 2)

        @pl.when((near >= 0) & (near < nz))
        def _():
            consume(near, 1)

        fwd(2 * t + 1)

        @pl.when((near >= 0) & (near < nz))
        def _():
            consume(far, 1)

        @pl.when(2 * t + 2 < nz)
        def _():
            fwd(2 * t + 2)

        return carry

    lax.fori_loop(1, nz // 2, tail, 0)

    chip = x * 2 + y
    for p in range(per):
        for r in range(CHIPS):
            @pl.when(jnp.logical_not((chip == r) & (c == p % 2)))
            def _():
                pltpu.make_async_remote_copy(
                    src_ref=ssend.at[0, 0], dst_ref=srecv.at[r, p], send_sem=s_ss.at[0, 0], recv_sem=s_rs.at[r, p],
                    device_id=(b, mate), device_id_type=MESH).wait_recv()
        total = own[p]
        for r in range(CHIPS):
            total = total + srecv[r, p].astype(F32)
        for i, each in enumerate(unpack(total, rows)):
            out[i, :, p * rows : (p + 1) * rows] = each

    def sent(zs, carry):
        for i in parts:
            @pl.when((zs <= z) & (z < nz - 1))
            def _():
                send(zs, i, b, up_sem.at[zs, i]).wait_send()

            @pl.when((zs >= z) & (z > 0))
            def _():
                send(zs, i, b, dn_sem.at[zs, i]).wait_send()

        q = (zs * NX + c) // per
        for v in range(NX):
            @pl.when((q != g) | (x != v))
            def _():
                pltpu.make_async_remote_copy(
                    src_ref=ssend.at[zs, v], dst_ref=srecv.at[0, 0], send_sem=s_ss.at[zs, v], recv_sem=s_rs.at[0, 0],
                    device_id=(b, mate), device_id_type=MESH).wait_send()

        return carry

    lax.fori_loop(0, nz, sent, 0)

    @pl.when(crossed)
    def _():
        for i in parts:
            swap(i).wait_send()

    for j in range(4):
        d_copy(j).wait_send()
    for h in range(CUTS):
        for j in range(2):
            y_copy(j, h).wait_send()
            l_copy(j, x, h).wait_send()
        x_copy(h).wait_send()


def solution(mesh):
    nb, ng = mesh.shape["band"], mesh.shape["ga"]
    nz = nb // NX
    per = nb // ng

    def step(elements, screened, energies, freq_points, freq_weights, band_of_slot):
        _, rows, depth = elements.shape
        slots = energies.shape[0]
        pad = -(-rows // 128) * 128
        cut = 2 * rows // CUTS
        packed = (3 * rows // 2, LANES) if packs(rows) else (2 * rows, rows)
        any_space = pl.BlockSpec(memory_space=pl.ANY)
        vmem = pl.BlockSpec(memory_space=pltpu.VMEM)
        dma = pltpu.SemaphoreType.DMA
        return pl.pallas_call(
            functools.partial(kernel, nb, ng),
            out_shape=pltpu.VMEM((2, rows, per * rows), F32),
            in_specs=[any_space] * 6,
            out_specs=vmem,
            scratch_shapes=[
                pltpu.VMEM((slots,), F32), pltpu.VMEM((slots,), jnp.int32),
                pltpu.SMEM(freq_points.shape, F32), pltpu.SMEM(freq_weights.shape, F32),
                pltpu.VMEM((2, rows, depth), BF16),
                pltpu.VMEM((2, nz * pad, depth), BF16),
                pltpu.VMEM((2, 4, 2, depth, depth), BF16),
                pltpu.VMEM((2 * rows, 2 * depth), BF16),
                pltpu.VMEM((16, slots), BF16),
                pltpu.VMEM((nb, 2, rows), F32),
                pltpu.VMEM((2, CUTS, cut, depth), F32),
                pltpu.VMEM((4, 2 * rows, depth), BF16),
                pltpu.VMEM((4, 2 * rows, depth), BF16),
                pltpu.VMEM((2, CUTS, cut, depth), BF16),
                pltpu.VMEM((2, CUTS, cut, depth), BF16),
                pltpu.VMEM((CUTS, cut, depth), BF16),
                pltpu.VMEM((NX, 2, CUTS, cut, depth), BF16),
                pltpu.VMEM((NX, 2, CUTS, cut, depth), BF16),
                pltpu.VMEM((nz, NX) + packed, BF16),
                pltpu.VMEM((CHIPS, per) + packed, BF16),
                pltpu.VMEM((per,) + packed, F32),
                dma((4,)), dma((2,)), dma((2, 4)), dma((4,)), dma((nz, 4)), dma((nz, 4)), dma((nz, 4)),
                dma((4,)), dma((4,)), dma((2, CUTS)), dma((2, CUTS)), dma((CUTS,)), dma((CUTS,)), dma((2, CUTS)), dma((2, CUTS)),
                dma((nz, NX)), dma((CHIPS, per)),
            ],
            compiler_params=pltpu.CompilerParams(
                collective_id=0, has_side_effects=True, vmem_limit_bytes=60 * 1024 * 1024),
        )(elements, screened, energies, band_of_slot, freq_points, freq_weights)

    placed = (P(None, "band", "ga"), P(None, None, "ga", None), P(), P(), P(), P())
    return jax.shard_map(
        step, mesh=mesh, in_specs=placed, out_specs=P(None, "band", "ga"), check_vma=False
    )
```

```python
import functools

import jax
import jax.numpy as jnp
from jax import lax
from jax.experimental import pallas as pl
from jax.experimental.pallas import tpu as pltpu
from jax.sharding import PartitionSpec as P

MESH = pl.DeviceIdType.MESH
F32 = jnp.float32
BF16 = jnp.bfloat16
NT = (((1,), (1,)), ((), ()))
NX = 2
CUTS = 4
LANES = 128
CHIPS = 4


def packs(rows):
    return 2 * (2 * rows - LANES) == LANES


def pack(re, im):
    rows = re.shape[0]
    if not packs(rows):
        return jnp.concatenate([re, im], axis=0)
    spare = LANES - rows
    top = jnp.concatenate([re, im[:, :spare]], axis=1)
    rest = im[:, spare:]
    return jnp.concatenate([top, jnp.concatenate([rest[: rows // 2], rest[rows // 2 :]], axis=1)], axis=0)


def unpack(both, rows):
    if not packs(rows):
        return both[:rows], both[rows:]
    rest = both[rows:]
    rest = jnp.concatenate([rest[:, : LANES // 2], rest[:, LANES // 2 :]], axis=0)
    return both[:rows, :rows], jnp.concatenate([both[:rows, rows:], rest], axis=1)


def kernel(nb, ng, el, wh, en_h, bos_h, fp_h, fw_h, out, *scratch):
    (en, bos, fp, fw, mine, gat, wv, a_ref, e3, scr, held, dsend, drecv, ysend, yrecv, xsend, lv, lw, ssend, srecv, own,
     in_sem, loc_sem, w_sem, sw_ss, up_sem, dn_sem, g_recv, d_ss, d_rs, y_ss, y_rs, x_ss, x_rs, l_ss, l_rs, s_ss,
     s_rs) = scratch
    rows, depth = el.shape[1], el.shape[2]
    nz = nb // NX
    pad = gat.shape[1] // nz
    cut = 2 * rows // CUTS
    per = nb // ng
    slots = en.shape[0]
    b, g = lax.axis_index("band"), lax.axis_index("ga")
    z, x = b // NX, lax.rem(b, NX)
    y, c = g // 2, lax.rem(g, 2)
    mate = g + 1 - 2 * c
    across = lax.rem(g + 2, ng)
    xb = b + 1 - 2 * x
    straight = x == c
    crossed = x != c

    barrier = pltpu.get_barrier_semaphore()

    def greet(band, ga):
        pl.semaphore_signal(barrier, inc=1, device_id=(band, ga), device_id_type=MESH)

    @pl.when(z > 0)
    def _():
        greet(b - NX, g)

    @pl.when(z < nz - 1)
    def _():
        greet(b + NX, g)

    greet(xb, g)
    greet(xb, mate)
    for r in range(1, ng):
        greet(b, lax.rem(g + r, ng))

    small = [pltpu.make_async_copy(s, t, in_sem.at[i]) for i, (s, t) in enumerate(
        ((en_h, en), (bos_h, bos), (fp_h, fp), (fw_h, fw)))]
    local = pltpu.make_async_copy(el, mine, loc_sem.at[0])
    local.start()

    def placed():
        return pltpu.make_async_copy(el, gat.at[:, pl.ds(pl.multiple_of(z * pad, pad), rows), :], loc_sem.at[1])

    @pl.when(straight)
    def _():
        placed().start()

    for copy in small:
        copy.start()

    def slice_of(j):
        ys = lax.rem(y + 1 - j // 2, 2)
        xs = lax.rem(x + 1 + j, 2)
        return ys * 2 + xs

    def w_copy(j, o):
        w = c if o else 1 - c
        cols = pl.ds(pl.multiple_of(slice_of(j) * depth, depth), depth)
        return pltpu.make_async_copy(wh.at[w, :, :, cols], wv.at[o, j], w_sem.at[o, j])

    def load(j, carry):
        for o in range(2):
            w_copy(j, o).start()
        return carry

    lax.fori_loop(0, 4, load, 0)
    local.wait()

    @pl.when(straight)
    def _():
        placed().wait()

    below = jnp.where(z > 0, 1, 0)
    above = jnp.where(z < nz - 1, 1, 0)
    pl.semaphore_wait(barrier, ng + 1 + below + above)

    unit = rows // 6
    pieces = ((0, unit), (unit, 2 * unit), (3 * unit, 2 * unit), (5 * unit, unit))
    parts = range(len(pieces))

    def block(zs, i):
        start, size = pieces[i]
        return gat.at[:, pl.ds(pl.multiple_of(zs * pad + start, unit), size), :]

    def send(zs, i, band, sem):
        ref = block(zs, i)
        return pltpu.make_async_remote_copy(
            src_ref=ref, dst_ref=ref, send_sem=sem, recv_sem=g_recv.at[zs, i], device_id=(band, g), device_id_type=MESH)

    def swap(i):
        start, size = pieces[i]
        return pltpu.make_async_remote_copy(
            src_ref=mine.at[:, pl.ds(start, size), :], dst_ref=block(z, i), send_sem=sw_ss.at[i],
            recv_sem=g_recv.at[z, i], device_id=(xb, mate), device_id_type=MESH)

    def arrived(zs, i):
        send(zs, i, b, up_sem.at[zs, i]).wait_recv()

    def send_z(zs, i, up, down):
        if up:
            @pl.when(z < nz - 1)
            def _():
                send(zs, i, b + NX, up_sem.at[zs, i]).start()

        if down:
            @pl.when(z > 0)
            def _():
                send(zs, i, b - NX, dn_sem.at[zs, i]).start()

    def fwd(s, which=parts, ways=(True, False)):
        for i in which:
            for up in ways:
                zs = z - s if up else z + s

                @pl.when((zs >= 0) & (zs < nz))
                def _():
                    arrived(zs, i)
                    send_z(zs, i, up, not up)

    def swapped(which):
        @pl.when(crossed)
        def _():
            for i in which:
                arrived(z, i)
                send_z(z, i, True, True)

    def early(which):
        @pl.when(straight)
        def _():
            fwd(1, which, (True,))

    @pl.when(straight)
    def _():
        for i in parts:
            send_z(z, i, True, True)

    @pl.when(crossed)
    def _():
        for i in parts:
            swap(i).start()

    er = mine[0]
    ei = mine[1]
    a_ref[:rows, :depth] = er
    a_ref[:rows, depth:] = ei
    a_ref[rows:, :depth] = -ei
    a_ref[rows:, depth:] = er

    def d_copy(j):
        return pltpu.make_async_remote_copy(
            src_ref=dsend.at[j], dst_ref=drecv.at[j], send_sem=d_ss.at[j], recv_sem=d_rs.at[j],
            device_id=(b, mate), device_id_type=MESH)

    def y_copy(j, h):
        return pltpu.make_async_remote_copy(
            src_ref=ysend.at[j, h], dst_ref=yrecv.at[j, h], send_sem=y_ss.at[j, h], recv_sem=y_rs.at[j, h],
            device_id=(b, across), device_id_type=MESH)

    def x_copy(h):
        return pltpu.make_async_remote_copy(
            src_ref=xsend.at[h], dst_ref=lv.at[x, c, h], send_sem=x_ss.at[h], recv_sem=x_rs.at[h],
            device_id=(xb, g), device_id_type=MESH)

    def l_copy(v, band, h):
        ref = lv.at[band, c, h]
        return pltpu.make_async_remote_copy(
            src_ref=ref, dst_ref=ref, send_sem=l_ss.at[v, h], recv_sem=l_rs.at[v, h],
            device_id=(b, mate), device_id_type=MESH)

    def first(j, o):
        w_copy(j, o).wait()
        part = jnp.dot(a_ref[...], wv[o, j].reshape(2 * depth, depth), preferred_element_type=F32)
        if not o:
            dsend[j] = part.astype(BF16)
            d_copy(j).start()
            return
        d_copy(j).wait_recv()
        part = part + drecv[j].astype(F32)
        for h in range(CUTS):
            if j < 2:
                ysend[j, h] = part[h * cut : (h + 1) * cut].astype(BF16)
                y_copy(j, h).start()
            else:
                held[j - 2, h] = part[h * cut : (h + 1) * cut]

    def to_x(h):
        y_copy(0, h).wait_recv()
        xsend[h] = (held[0, h] + yrecv[0, h].astype(F32)).astype(BF16)
        x_copy(h).start()

    def here(h):
        y_copy(1, h).wait_recv()
        lv[x, c, h] = (held[1, h] + yrecv[1, h].astype(F32)).astype(BF16)
        l_copy(0, x, h).start()

    def from_x(h):
        x_copy(h).wait_recv()
        l_copy(1, 1 - x, h).start()

    def ready(other):
        half = CUTS // 2
        v = 1 - x if other else x
        for h in range(CUTS):
            l_copy(other, x, h).wait_recv()
        for w in range(2):
            lw[v, w, :half] = -lv[v, w, half:]
            lw[v, w, half:] = lv[v, w, :half]

    def consume(zs, count, v=None):
        at = pl.ds(pl.multiple_of(zs * pad, pad), count * pad)
        bands = range(NX) if v is None else (v,)
        left, right = [ref[...] if v is None else ref[v] for ref in (lv, lw)]
        shape = (4 * len(bands) * rows, depth)
        pr = lax.dot_general(left.reshape(shape), gat[0, at, :], NT, preferred_element_type=F32)
        pr = pr + lax.dot_general(right.reshape(shape), gat[1, at, :], NT, preferred_element_type=F32)
        for t in range(count):
            for n, band in enumerate(bands):
                scale_and_send(zs + t, band, [
                    pr[(4 * n + i) * rows : (4 * n + i + 1) * rows, t * pad : t * pad + rows] for i in range(4)])

    def scale_and_send(zs, v, each):
        k = zs * NX + c
        q, p = k // per, lax.rem(k, per)
        col = [jnp.where(v == 0, cols[0][w], cols[1][w]) for w in range(2)]
        f = [col[w] + scr[k, w : w + 1, :] for w in range(2)]
        total = [f[0] * each[i] + f[1] * each[2 + i] for i in range(2)]
        home = (q == g) & (x == v)

        @pl.when(home)
        def _():
            own[p] = pack(*total)
            srecv[x * 2 + y, p] = jnp.zeros(srecv.shape[2:], BF16)

        @pl.when(jnp.logical_not(home))
        def _():
            ssend[zs, v] = pack(*[part.astype(BF16) for part in total])
            pltpu.make_async_remote_copy(
                src_ref=ssend.at[zs, v], dst_ref=srecv.at[x * 2 + y, p], send_sem=s_ss.at[zs, v],
                recv_sem=s_rs.at[x * 2 + y, p], device_id=(z * NX + v, q), device_id_type=MESH).start()

    first(0, 0)
    first(1, 0)

    for copy in small:
        copy.wait()
    row = lax.broadcasted_iota(jnp.int32, (16, slots), 0)
    e = en[...].reshape(1, slots)
    hi = e.astype(BF16).astype(F32)
    mid = (e - hi).astype(BF16).astype(F32)
    lo = e - hi - mid
    e3[...] = jnp.where(row == 0, hi, jnp.where(row == 1, mid, jnp.where(row == 2, lo, 0.0))).astype(BF16)
    tile = slots if slots <= 1024 else 8 * rows

    for u in range(slots // tile):
        slot = bos[u * tile : (u + 1) * tile].reshape(1, tile)

        def add(j, acc):
            at = pl.multiple_of(j * tile, tile)
            hit = lax.broadcasted_iota(jnp.int32, (tile, tile), 0) + at == slot
            return acc + jnp.dot(e3[:, pl.ds(at, tile)], jnp.where(hit, 1.0, 0.0).astype(BF16),
                                 preferred_element_type=F32)

        acc = lax.fori_loop(0, slots // tile, add, jnp.zeros((16, tile), F32))
        energy = jnp.sum(acc, axis=0, keepdims=True)
        for w in range(2):
            off = energy - fp[w]
            value = 0.5 * (fw[w] / (1.0 + 4.0 * off * off))
            for v in range(tile // rows):
                scr[u * (tile // rows) + v, w : w + 1, :] = value[:, v * rows : (v + 1) * rows]
    pick = lax.broadcasted_iota(jnp.int32, (rows, rows), 1) == lax.broadcasted_iota(
        jnp.int32, (rows, rows), 0)
    cols = [[jnp.sum(jnp.where(pick, scr[band, w : w + 1, :], 0.0), axis=1, keepdims=True)
             for w in range(2)] for band in (z * NX, z * NX + 1)]

    first(0, 1)
    first(1, 1)
    first(2, 0)
    swapped((0,))
    first(3, 0)
    swapped((1, 2, 3))
    early((0, 1))
    first(2, 1)
    first(3, 1)
    own[...] = jnp.zeros(own.shape, F32)

    @pl.when(straight)
    def _():
        fwd(1, (0, 1), (False,))
        to_x(0)
        fwd(1, (2, 3))
        to_x(1)
        to_x(2)
        to_x(3)
        fwd(2, (0, 1))
        here(0)
        from_x(0)
        fwd(2, (2,))
        here(1)
        from_x(1)
        fwd(2, (3,))

    @pl.when(crossed)
    def _():
        to_x(0)
        to_x(1)
        fwd(1, (0, 1))
        to_x(2)
        fwd(1, (2,))
        to_x(3)
        fwd(1, (3,))
        here(0)
        from_x(0)
        here(1)
        from_x(1)

    even = lax.rem(z, 2) == 0
    edge = (z == 0) | (z == nz - 1)

    @pl.when(crossed & jnp.logical_not(edge))
    def _():
        fwd(2, (0, 1))

    from_x(2)
    from_x(3)
    here(2)

    @pl.when(crossed & jnp.logical_not(edge))
    def _():
        fwd(2, (2, 3))

    here(3)

    for other in (1, 0):
        ready(other)
        v = 1 - x if other else x

        @pl.when(even & (z > 0))
        def _():
            consume(z - 2, 2, v)

        consume(z // 2 * 2, 2, v)

        @pl.when(jnp.logical_not(even) & (z < nz - 1))
        def _():
            consume(z + 1, 2, v)

    @pl.when(crossed & edge)
    def _():
        fwd(2)

    def tail(t, carry):
        base = z // 2 * 2
        inner = base + jnp.where(even, -2 * t, 2 * t)
        near = jnp.where(even, base + 2 * t, base - 2 * t + 1)
        far = jnp.where(even, near + 1, near - 1)

        @pl.when((t > 1) & (inner >= 0) & (inner < nz))
        def _():
            consume(inner, 2)

        @pl.when((near >= 0) & (near < nz))
        def _():
            consume(near, 1)

        fwd(2 * t + 1)

        @pl.when((near >= 0) & (near < nz))
        def _():
            consume(far, 1)

        @pl.when(2 * t + 2 < nz)
        def _():
            fwd(2 * t + 2)

        return carry

    lax.fori_loop(1, nz // 2, tail, 0)

    chip = x * 2 + y
    for p in range(per):
        for r in range(CHIPS):
            @pl.when(jnp.logical_not((chip == r) & (c == p % 2)))
            def _():
                pltpu.make_async_remote_copy(
                    src_ref=ssend.at[0, 0], dst_ref=srecv.at[r, p], send_sem=s_ss.at[0, 0], recv_sem=s_rs.at[r, p],
                    device_id=(b, mate), device_id_type=MESH).wait_recv()
        total = own[p]
        for r in range(CHIPS):
            total = total + srecv[r, p].astype(F32)
        for i, each in enumerate(unpack(total, rows)):
            out[i, :, p * rows : (p + 1) * rows] = each

    def sent(zs, carry):
        for i in parts:
            @pl.when((zs <= z) & (z < nz - 1))
            def _():
                send(zs, i, b, up_sem.at[zs, i]).wait_send()

            @pl.when((zs >= z) & (z > 0))
            def _():
                send(zs, i, b, dn_sem.at[zs, i]).wait_send()

        q = (zs * NX + c) // per
        for v in range(NX):
            @pl.when((q != g) | (x != v))
            def _():
                pltpu.make_async_remote_copy(
                    src_ref=ssend.at[zs, v], dst_ref=srecv.at[0, 0], send_sem=s_ss.at[zs, v], recv_sem=s_rs.at[0, 0],
                    device_id=(b, mate), device_id_type=MESH).wait_send()

        return carry

    lax.fori_loop(0, nz, sent, 0)

    @pl.when(crossed)
    def _():
        for i in parts:
            swap(i).wait_send()

    for j in range(4):
        d_copy(j).wait_send()
    for h in range(CUTS):
        for j in range(2):
            y_copy(j, h).wait_send()
            l_copy(j, x, h).wait_send()
        x_copy(h).wait_send()


def solution(mesh):
    nb, ng = mesh.shape["band"], mesh.shape["ga"]
    nz = nb // NX
    per = nb // ng

    def step(elements, screened, energies, freq_points, freq_weights, band_of_slot):
        _, rows, depth = elements.shape
        slots = energies.shape[0]
        pad = -(-rows // 128) * 128
        cut = 2 * rows // CUTS
        packed = (3 * rows // 2, LANES) if packs(rows) else (2 * rows, rows)
        any_space = pl.BlockSpec(memory_space=pl.ANY)
        vmem = pl.BlockSpec(memory_space=pltpu.VMEM)
        dma = pltpu.SemaphoreType.DMA
        return pl.pallas_call(
            functools.partial(kernel, nb, ng),
            out_shape=pltpu.VMEM((2, rows, per * rows), F32),
            in_specs=[any_space] * 6,
            out_specs=vmem,
            scratch_shapes=[
                pltpu.VMEM((slots,), F32), pltpu.VMEM((slots,), jnp.int32),
                pltpu.SMEM(freq_points.shape, F32), pltpu.SMEM(freq_weights.shape, F32),
                pltpu.VMEM((2, rows, depth), BF16),
                pltpu.VMEM((2, nz * pad, depth), BF16),
                pltpu.VMEM((2, 4, 2, depth, depth), BF16),
                pltpu.VMEM((2 * rows, 2 * depth), BF16),
                pltpu.VMEM((16, slots), BF16),
                pltpu.VMEM((nb, 2, rows), F32),
                pltpu.VMEM((2, CUTS, cut, depth), F32),
                pltpu.VMEM((4, 2 * rows, depth), BF16),
                pltpu.VMEM((4, 2 * rows, depth), BF16),
                pltpu.VMEM((2, CUTS, cut, depth), BF16),
                pltpu.VMEM((2, CUTS, cut, depth), BF16),
                pltpu.VMEM((CUTS, cut, depth), BF16),
                pltpu.VMEM((NX, 2, CUTS, cut, depth), BF16),
                pltpu.VMEM((NX, 2, CUTS, cut, depth), BF16),
                pltpu.VMEM((nz, NX) + packed, BF16),
                pltpu.VMEM((CHIPS, per) + packed, BF16),
                pltpu.VMEM((per,) + packed, F32),
                dma((4,)), dma((2,)), dma((2, 4)), dma((4,)), dma((nz, 4)), dma((nz, 4)), dma((nz, 4)),
                dma((4,)), dma((4,)), dma((2, CUTS)), dma((2, CUTS)), dma((CUTS,)), dma((CUTS,)), dma((2, CUTS)), dma((2, CUTS)),
                dma((nz, NX)), dma((CHIPS, per)),
            ],
            compiler_params=pltpu.CompilerParams(
                collective_id=0, has_side_effects=True, vmem_limit_bytes=60 * 1024 * 1024),
        )(elements, screened, energies, band_of_slot, freq_points, freq_weights)

    placed = (P(None, "band", "ga"), P(None, None, "ga", None), P(), P(), P(), P())
    return jax.shard_map(
        step, mesh=mesh, in_specs=placed, out_specs=P(None, "band", "ga"), check_vma=False
    )
```

```python
import functools

import jax
import jax.numpy as jnp
from jax import lax
from jax.experimental import pallas as pl
from jax.experimental.pallas import tpu as pltpu
from jax.sharding import PartitionSpec as P

MESH = pl.DeviceIdType.MESH
F32 = jnp.float32
BF16 = jnp.bfloat16
NT = (((1,), (1,)), ((), ()))
NX = 2
CUTS = 4
LANES = 128
CHIPS = 4


def packs(rows):
    return 2 * (2 * rows - LANES) == LANES


def pack(re, im):
    rows = re.shape[0]
    if not packs(rows):
        return jnp.concatenate([re, im], axis=0)
    spare = LANES - rows
    top = jnp.concatenate([re, im[:, :spare]], axis=1)
    rest = im[:, spare:]
    return jnp.concatenate([top, jnp.concatenate([rest[: rows // 2], rest[rows // 2 :]], axis=1)], axis=0)


def unpack(both, rows):
    if not packs(rows):
        return both[:rows], both[rows:]
    rest = both[rows:]
    rest = jnp.concatenate([rest[:, : LANES // 2], rest[:, LANES // 2 :]], axis=0)
    return both[:rows, :rows], jnp.concatenate([both[:rows, rows:], rest], axis=1)


def kernel(nb, ng, el, wh, en_h, bos_h, fp_h, fw_h, out, *scratch):
    (en, bos, fp, fw, mine, gat, wv, a_ref, e3, scr, held, dsend, drecv, ysend, yrecv, xsend, lv, lw, ssend, srecv, own,
     in_sem, loc_sem, w_sem, sw_ss, up_sem, dn_sem, g_recv, d_ss, d_rs, y_ss, y_rs, x_ss, x_rs, l_ss, l_rs, s_ss,
     s_rs) = scratch
    rows, depth = el.shape[1], el.shape[2]
    nz = nb // NX
    pad = gat.shape[1] // nz
    cut = 2 * rows // CUTS
    per = nb // ng
    slots = en.shape[0]
    b, g = lax.axis_index("band"), lax.axis_index("ga")
    z, x = b // NX, lax.rem(b, NX)
    y, c = g // 2, lax.rem(g, 2)
    mate = g + 1 - 2 * c
    across = lax.rem(g + 2, ng)
    xb = b + 1 - 2 * x
    straight = x == c
    crossed = x != c

    barrier = pltpu.get_barrier_semaphore()

    def greet(band, ga):
        pl.semaphore_signal(barrier, inc=1, device_id=(band, ga), device_id_type=MESH)

    @pl.when(z > 0)
    def _():
        greet(b - NX, g)

    @pl.when(z < nz - 1)
    def _():
        greet(b + NX, g)

    greet(xb, g)
    greet(xb, mate)
    for r in range(1, ng):
        greet(b, lax.rem(g + r, ng))

    small = [pltpu.make_async_copy(s, t, in_sem.at[i]) for i, (s, t) in enumerate(
        ((en_h, en), (bos_h, bos), (fp_h, fp), (fw_h, fw)))]
    local = pltpu.make_async_copy(el, mine, loc_sem.at[0])
    local.start()

    def placed():
        return pltpu.make_async_copy(el, gat.at[:, pl.ds(pl.multiple_of(z * pad, pad), rows), :], loc_sem.at[1])

    @pl.when(straight)
    def _():
        placed().start()

    for copy in small:
        copy.start()

    def slice_of(j):
        ys = lax.rem(y + 1 - j // 2, 2)
        xs = lax.rem(x + 1 + j, 2)
        return ys * 2 + xs

    def w_copy(j, o):
        w = c if o else 1 - c
        cols = pl.ds(pl.multiple_of(slice_of(j) * depth, depth), depth)
        return pltpu.make_async_copy(wh.at[w, :, :, cols], wv.at[o, j], w_sem.at[o, j])

    def load(j, carry):
        for o in range(2):
            w_copy(j, o).start()
        return carry

    lax.fori_loop(0, 4, load, 0)
    local.wait()

    @pl.when(straight)
    def _():
        placed().wait()

    below = jnp.where(z > 0, 1, 0)
    above = jnp.where(z < nz - 1, 1, 0)
    pl.semaphore_wait(barrier, ng + 1 + below + above)

    unit = rows // 6
    pieces = ((0, 2 * unit), (2 * unit, 2 * unit), (4 * unit, unit), (5 * unit, unit))
    parts = range(len(pieces))

    def block(zs, i):
        start, size = pieces[i]
        return gat.at[:, pl.ds(pl.multiple_of(zs * pad + start, unit), size), :]

    def send(zs, i, band, sem):
        ref = block(zs, i)
        return pltpu.make_async_remote_copy(
            src_ref=ref, dst_ref=ref, send_sem=sem, recv_sem=g_recv.at[zs, i], device_id=(band, g), device_id_type=MESH)

    def swap(i):
        start, size = pieces[i]
        return pltpu.make_async_remote_copy(
            src_ref=mine.at[:, pl.ds(start, size), :], dst_ref=block(z, i), send_sem=sw_ss.at[i],
            recv_sem=g_recv.at[z, i], device_id=(xb, mate), device_id_type=MESH)

    def arrived(zs, i):
        send(zs, i, b, up_sem.at[zs, i]).wait_recv()

    def send_z(zs, i, up, down):
        if up:
            @pl.when(z < nz - 1)
            def _():
                send(zs, i, b + NX, up_sem.at[zs, i]).start()

        if down:
            @pl.when(z > 0)
            def _():
                send(zs, i, b - NX, dn_sem.at[zs, i]).start()

    def fwd(s, which=parts, ways=(True, False)):
        for i in which:
            for up in ways:
                zs = z - s if up else z + s

                @pl.when((zs >= 0) & (zs < nz))
                def _():
                    arrived(zs, i)
                    send_z(zs, i, up, not up)

    def swapped(which):
        @pl.when(crossed)
        def _():
            for i in which:
                arrived(z, i)
                send_z(z, i, True, True)

    def early(which):
        @pl.when(straight)
        def _():
            fwd(1, which, (True,))

    @pl.when(straight)
    def _():
        for i in parts:
            send_z(z, i, True, True)

    @pl.when(crossed)
    def _():
        for i in parts:
            swap(i).start()

    er = mine[0]
    ei = mine[1]
    a_ref[:rows, :depth] = er
    a_ref[:rows, depth:] = ei
    a_ref[rows:, :depth] = -ei
    a_ref[rows:, depth:] = er

    def d_copy(j):
        return pltpu.make_async_remote_copy(
            src_ref=dsend.at[j], dst_ref=drecv.at[j], send_sem=d_ss.at[j], recv_sem=d_rs.at[j],
            device_id=(b, mate), device_id_type=MESH)

    def y_copy(j, h):
        return pltpu.make_async_remote_copy(
            src_ref=ysend.at[j, h], dst_ref=yrecv.at[j, h], send_sem=y_ss.at[j, h], recv_sem=y_rs.at[j, h],
            device_id=(b, across), device_id_type=MESH)

    def x_copy(h):
        return pltpu.make_async_remote_copy(
            src_ref=xsend.at[h], dst_ref=lv.at[x, c, h], send_sem=x_ss.at[h], recv_sem=x_rs.at[h],
            device_id=(xb, g), device_id_type=MESH)

    def l_copy(v, band, h):
        ref = lv.at[band, c, h]
        return pltpu.make_async_remote_copy(
            src_ref=ref, dst_ref=ref, send_sem=l_ss.at[v, h], recv_sem=l_rs.at[v, h],
            device_id=(b, mate), device_id_type=MESH)

    def first(j, o):
        w_copy(j, o).wait()
        part = jnp.dot(a_ref[...], wv[o, j].reshape(2 * depth, depth), preferred_element_type=F32)
        if not o:
            dsend[j] = part.astype(BF16)
            d_copy(j).start()
            return
        d_copy(j).wait_recv()
        part = part + drecv[j].astype(F32)
        for h in range(CUTS):
            if j < 2:
                ysend[j, h] = part[h * cut : (h + 1) * cut].astype(BF16)
                y_copy(j, h).start()
            else:
                held[j - 2, h] = part[h * cut : (h + 1) * cut]

    def to_x(h):
        y_copy(0, h).wait_recv()
        xsend[h] = (held[0, h] + yrecv[0, h].astype(F32)).astype(BF16)
        x_copy(h).start()

    def here(h):
        y_copy(1, h).wait_recv()
        lv[x, c, h] = (held[1, h] + yrecv[1, h].astype(F32)).astype(BF16)
        l_copy(0, x, h).start()

    def from_x(h):
        x_copy(h).wait_recv()
        l_copy(1, 1 - x, h).start()

    def ready(other):
        half = CUTS // 2
        v = 1 - x if other else x
        for h in range(CUTS):
            l_copy(other, x, h).wait_recv()
        for w in range(2):
            lw[v, w, :half] = -lv[v, w, half:]
            lw[v, w, half:] = lv[v, w, :half]

    def consume(zs, count, v=None):
        at = pl.ds(pl.multiple_of(zs * pad, pad), count * pad)
        bands = range(NX) if v is None else (v,)
        left, right = [ref[...] if v is None else ref[v] for ref in (lv, lw)]
        shape = (4 * len(bands) * rows, depth)
        pr = lax.dot_general(left.reshape(shape), gat[0, at, :], NT, preferred_element_type=F32)
        pr = pr + lax.dot_general(right.reshape(shape), gat[1, at, :], NT, preferred_element_type=F32)
        for t in range(count):
            for n, band in enumerate(bands):
                scale_and_send(zs + t, band, [
                    pr[(4 * n + i) * rows : (4 * n + i + 1) * rows, t * pad : t * pad + rows] for i in range(4)])

    def scale_and_send(zs, v, each):
        k = zs * NX + c
        q, p = k // per, lax.rem(k, per)
        col = [jnp.where(v == 0, cols[0][w], cols[1][w]) for w in range(2)]
        f = [col[w] + scr[k, w : w + 1, :] for w in range(2)]
        total = [f[0] * each[i] + f[1] * each[2 + i] for i in range(2)]
        home = (q == g) & (x == v)

        @pl.when(home)
        def _():
            own[p] = pack(*total)
            srecv[x * 2 + y, p] = jnp.zeros(srecv.shape[2:], BF16)

        @pl.when(jnp.logical_not(home))
        def _():
            ssend[zs, v] = pack(*[part.astype(BF16) for part in total])
            pltpu.make_async_remote_copy(
                src_ref=ssend.at[zs, v], dst_ref=srecv.at[x * 2 + y, p], send_sem=s_ss.at[zs, v],
                recv_sem=s_rs.at[x * 2 + y, p], device_id=(z * NX + v, q), device_id_type=MESH).start()

    first(0, 0)
    first(1, 0)

    for copy in small:
        copy.wait()
    row = lax.broadcasted_iota(jnp.int32, (16, slots), 0)
    e = en[...].reshape(1, slots)
    hi = e.astype(BF16).astype(F32)
    mid = (e - hi).astype(BF16).astype(F32)
    lo = e - hi - mid
    e3[...] = jnp.where(row == 0, hi, jnp.where(row == 1, mid, jnp.where(row == 2, lo, 0.0))).astype(BF16)
    tile = slots if slots <= 1024 else 8 * rows

    for u in range(slots // tile):
        slot = bos[u * tile : (u + 1) * tile].reshape(1, tile)

        def add(j, acc):
            at = pl.multiple_of(j * tile, tile)
            hit = lax.broadcasted_iota(jnp.int32, (tile, tile), 0) + at == slot
            return acc + jnp.dot(e3[:, pl.ds(at, tile)], jnp.where(hit, 1.0, 0.0).astype(BF16),
                                 preferred_element_type=F32)

        acc = lax.fori_loop(0, slots // tile, add, jnp.zeros((16, tile), F32))
        energy = jnp.sum(acc, axis=0, keepdims=True)
        for w in range(2):
            off = energy - fp[w]
            value = 0.5 * (fw[w] / (1.0 + 4.0 * off * off))
            for v in range(tile // rows):
                scr[u * (tile // rows) + v, w : w + 1, :] = value[:, v * rows : (v + 1) * rows]
    pick = lax.broadcasted_iota(jnp.int32, (rows, rows), 1) == lax.broadcasted_iota(
        jnp.int32, (rows, rows), 0)
    cols = [[jnp.sum(jnp.where(pick, scr[band, w : w + 1, :], 0.0), axis=1, keepdims=True)
             for w in range(2)] for band in (z * NX, z * NX + 1)]

    first(0, 1)
    first(1, 1)
    first(2, 0)
    swapped((0,))
    first(3, 0)
    swapped((1, 2, 3))
    early((0, 1))
    first(2, 1)
    first(3, 1)
    own[...] = jnp.zeros(own.shape, F32)

    @pl.when(straight)
    def _():
        fwd(1, (0, 1), (False,))
        to_x(0)
        fwd(1, (2, 3))
        to_x(1)
        to_x(2)
        to_x(3)
        fwd(2, (0, 1))
        here(0)
        from_x(0)
        fwd(2, (2,))
        here(1)
        from_x(1)
        fwd(2, (3,))

    @pl.when(crossed)
    def _():
        to_x(0)
        to_x(1)
        fwd(1, (0, 1))
        to_x(2)
        fwd(1, (2,))
        to_x(3)
        fwd(1, (3,))
        here(0)
        from_x(0)
        here(1)
        from_x(1)

    even = lax.rem(z, 2) == 0
    edge = (z == 0) | (z == nz - 1)

    @pl.when(crossed & jnp.logical_not(edge))
    def _():
        fwd(2, (0, 1))

    from_x(2)
    from_x(3)
    here(2)

    @pl.when(crossed & jnp.logical_not(edge))
    def _():
        fwd(2, (2, 3))

    here(3)

    beside = jnp.where(z == 0, 2, nz - 3)
    first_beside = edge & ((beside * NX + c) // per // 2 != y)

    @pl.when(crossed & first_beside)
    def _():
        fwd(2)

    for other in (1, 0):
        ready(other)
        v = 1 - x if other else x

        @pl.when(first_beside)
        def _():
            consume(beside, 1, v)

        @pl.when(even & (z > 0))
        def _():
            consume(z - 2, 2, v)

        consume(z // 2 * 2, 2, v)

        @pl.when(jnp.logical_not(even) & (z < nz - 1))
        def _():
            consume(z + 1, 2, v)

    @pl.when(crossed & edge & jnp.logical_not(first_beside))
    def _():
        fwd(2)

    def tail(t, carry):
        base = z // 2 * 2
        inner = base + jnp.where(even, -2 * t, 2 * t)
        near = jnp.where(even, base + 2 * t, base - 2 * t + 1)
        far = jnp.where(even, near + 1, near - 1)

        @pl.when((t > 1) & (inner >= 0) & (inner < nz))
        def _():
            consume(inner, 2)

        @pl.when((near >= 0) & (near < nz) & ((t > 1) | jnp.logical_not(first_beside)))
        def _():
            consume(near, 1)

        fwd(2 * t + 1)

        @pl.when((near >= 0) & (near < nz))
        def _():
            consume(far, 1)

        @pl.when(2 * t + 2 < nz)
        def _():
            fwd(2 * t + 2)

        return carry

    lax.fori_loop(1, nz // 2, tail, 0)

    chip = x * 2 + y
    for p in range(per):
        for r in range(CHIPS):
            @pl.when(jnp.logical_not((chip == r) & (c == p % 2)))
            def _():
                pltpu.make_async_remote_copy(
                    src_ref=ssend.at[0, 0], dst_ref=srecv.at[r, p], send_sem=s_ss.at[0, 0], recv_sem=s_rs.at[r, p],
                    device_id=(b, mate), device_id_type=MESH).wait_recv()
        total = own[p]
        for r in range(CHIPS):
            total = total + srecv[r, p].astype(F32)
        for i, each in enumerate(unpack(total, rows)):
            out[i, :, p * rows : (p + 1) * rows] = each

    def sent(zs, carry):
        for i in parts:
            @pl.when((zs <= z) & (z < nz - 1))
            def _():
                send(zs, i, b, up_sem.at[zs, i]).wait_send()

            @pl.when((zs >= z) & (z > 0))
            def _():
                send(zs, i, b, dn_sem.at[zs, i]).wait_send()

        q = (zs * NX + c) // per
        for v in range(NX):
            @pl.when((q != g) | (x != v))
            def _():
                pltpu.make_async_remote_copy(
                    src_ref=ssend.at[zs, v], dst_ref=srecv.at[0, 0], send_sem=s_ss.at[zs, v], recv_sem=s_rs.at[0, 0],
                    device_id=(b, mate), device_id_type=MESH).wait_send()

        return carry

    lax.fori_loop(0, nz, sent, 0)

    @pl.when(crossed)
    def _():
        for i in parts:
            swap(i).wait_send()

    for j in range(4):
        d_copy(j).wait_send()
    for h in range(CUTS):
        for j in range(2):
            y_copy(j, h).wait_send()
            l_copy(j, x, h).wait_send()
        x_copy(h).wait_send()


def solution(mesh):
    nb, ng = mesh.shape["band"], mesh.shape["ga"]
    nz = nb // NX
    per = nb // ng

    def step(elements, screened, energies, freq_points, freq_weights, band_of_slot):
        _, rows, depth = elements.shape
        slots = energies.shape[0]
        pad = -(-rows // 128) * 128
        cut = 2 * rows // CUTS
        packed = (3 * rows // 2, LANES) if packs(rows) else (2 * rows, rows)
        any_space = pl.BlockSpec(memory_space=pl.ANY)
        vmem = pl.BlockSpec(memory_space=pltpu.VMEM)
        dma = pltpu.SemaphoreType.DMA
        return pl.pallas_call(
            functools.partial(kernel, nb, ng),
            out_shape=pltpu.VMEM((2, rows, per * rows), F32),
            in_specs=[any_space] * 6,
            out_specs=vmem,
            scratch_shapes=[
                pltpu.VMEM((slots,), F32), pltpu.VMEM((slots,), jnp.int32),
                pltpu.SMEM(freq_points.shape, F32), pltpu.SMEM(freq_weights.shape, F32),
                pltpu.VMEM((2, rows, depth), BF16),
                pltpu.VMEM((2, nz * pad, depth), BF16),
                pltpu.VMEM((2, 4, 2, depth, depth), BF16),
                pltpu.VMEM((2 * rows, 2 * depth), BF16),
                pltpu.VMEM((16, slots), BF16),
                pltpu.VMEM((nb, 2, rows), F32),
                pltpu.VMEM((2, CUTS, cut, depth), F32),
                pltpu.VMEM((4, 2 * rows, depth), BF16),
                pltpu.VMEM((4, 2 * rows, depth), BF16),
                pltpu.VMEM((2, CUTS, cut, depth), BF16),
                pltpu.VMEM((2, CUTS, cut, depth), BF16),
                pltpu.VMEM((CUTS, cut, depth), BF16),
                pltpu.VMEM((NX, 2, CUTS, cut, depth), BF16),
                pltpu.VMEM((NX, 2, CUTS, cut, depth), BF16),
                pltpu.VMEM((nz, NX) + packed, BF16),
                pltpu.VMEM((CHIPS, per) + packed, BF16),
                pltpu.VMEM((per,) + packed, F32),
                dma((4,)), dma((2,)), dma((2, 4)), dma((4,)), dma((nz, 4)), dma((nz, 4)), dma((nz, 4)),
                dma((4,)), dma((4,)), dma((2, CUTS)), dma((2, CUTS)), dma((CUTS,)), dma((CUTS,)), dma((2, CUTS)), dma((2, CUTS)),
                dma((nz, NX)), dma((CHIPS, per)),
            ],
            compiler_params=pltpu.CompilerParams(
                collective_id=0, has_side_effects=True, vmem_limit_bytes=60 * 1024 * 1024),
        )(elements, screened, energies, band_of_slot, freq_points, freq_weights)

    placed = (P(None, "band", "ga"), P(None, None, "ga", None), P(), P(), P(), P())
    return jax.shard_map(
        step, mesh=mesh, in_specs=placed, out_specs=P(None, "band", "ga"), check_vma=False
    )
```
